512 devices in a mesh: scan: 2 (over y), ang: 32 (over z, core), row: 8 (over x).
Axes of the slice: x: 8, y: 2, z: 16, core: 2. Of those that a mesh axis runs over, the one named last changes fastest.
The devices are a block of a 8x16x16 slice.
Arguments:
- projections: bfloat16 [64, 64, 2560], P(('scan', 'ang'), 'row'), parts along dimension 0, may hold values from 0 to 2
- flats: float32 [128, 2560], P(('scan', 'row')), parts along dimension 0, may hold values from 1 to 3
- block_start: int32 [32, 32], replicated, may hold values from 0 to 2528
- bp_weights: bfloat16 [32, 32, 8192], P(None, None, 'ang'), may hold values from -0.1875 to 0.1875
Outputs:
- recon: float32 [128, 8192], P(('scan', 'row'), 'ang'), parts along dimension 0
The draws below stay inside these ranges and needn't reach their ends.
There are 2 independent parts, one for each index of `scan`. The reference program is written for one: setup_inputs(seed, part) draws one part's arguments, and reference() takes and returns one part's arrays. A program takes and returns all parts, laid end to end along the dimension named above; an argument that names none is the same for every part. Nothing has to cross between parts.
Inputs may be any that keep to these rules, and one draw needn't show every extreme that they name: block_start[a, r] is the first of the 32 detector columns that pixel region r reads at angle a.
All inputs are finite; a program needn't handle non-finite values.
Results may differ from the reference program's by a relative error of at most 0.009.
Values may be sent and summed in bfloat16 or wider, within the bound.
A program may use at most 64 MiB of HBM per device.

```python
import math
import jax
import jax.numpy as jnp
from jax import lax

W = 2560
RD = 8
HALO = 4
CB = 32
PIX_DEV = 256
TILE = 16
ANGLES = 32
SLICES = 64
REGIONS = 32
PIX = 8192


def set_ends(entries, stream_key, smallest, largest):
    shape = entries.shape
    spot = [jax.random.randint(jax.random.fold_in(stream_key, axis), (), 0, shape[axis]) for axis in range(len(shape))]
    entries = entries.at[tuple(spot)].set(smallest)
    longest = shape.index(max(shape))
    spot[longest] = (spot[longest] + 1) % shape[longest]
    return entries.at[tuple(spot)].set(largest)


def levels(rng, extent, shards, least, largest):
    factor_of = 1.0
    for position, shards_of in shards:
        steps = jax.random.uniform(jax.random.fold_in(jax.random.fold_in(rng, 6), position), (shards_of,), jnp.float32, least / len(shards), largest / len(shards))
        factor_of = factor_of * jnp.repeat(jnp.exp(steps), extent[position] // shards_of).reshape((-1,) + (1,) * (len(extent) - 1 - position))
    return factor_of


def gaussian(own_key, dims, scale, bound, shards=(), kind=jnp.bfloat16):
    array = jax.random.normal(own_key, dims, jnp.float32) * scale
    if len(shards) > 0:
        array = levels(own_key, dims, shards, -0.22, 0.18) * array
    return jnp.clip(array, min=-bound, max=bound).astype(kind)


def setup_inputs(seed: int = 0, part: int = 0) -> dict:
    keys = jax.random.split(jax.random.key(seed), 5)
    part_splits = jax.random.split(jax.random.fold_in(keys[4], part), 5)
    projections = jnp.clip(2.0 * jax.random.uniform(part_splits[0], (ANGLES, SLICES, W), jnp.float32) ** levels(part_splits[0], (ANGLES, SLICES, W), ((0, 32), (1, 8)), -0.2, 0.2), 0.0, 2.0).astype(jnp.bfloat16)
    flats = jnp.clip(jnp.exp(math.log(3.0) - 1.0986123 * jax.random.uniform(part_splits[1], (SLICES, W), jnp.float32) ** levels(part_splits[1], (SLICES, W), ((0, 8),), -0.2, 0.2)), 1.0, 3.0)
    block_start = set_ends(jax.random.randint(keys[2], (ANGLES, REGIONS), 0, W - CB + 1), jax.random.fold_in(keys[2], 1), 0, W - CB).astype(jnp.int32)
    bp_weights = gaussian(keys[3], (ANGLES, CB, PIX), (ANGLES * CB) ** -0.5, 0.1875, ((2, 32),))
    return dict(projections=projections, flats=flats, block_start=block_start, bp_weights=bp_weights)


paganin_beta = 8.0
ramp_gain = 320.0


def reference(projections, flats, block_start, bp_weights):
    contrast = 1.0 - projections.astype(jnp.float32) / flats[None, :, :]
    padded = jnp.pad(contrast, ((0, 0), (HALO, HALO), (0, 0)))
    tile_count = SLICES // RD
    row_index = (jnp.arange(tile_count, dtype=jnp.int32)[:, None] * RD
                 + jnp.arange(TILE, dtype=jnp.int32)[None, :]).astype(jnp.int32)
    row_freq = jnp.arange(TILE, dtype=jnp.float32)
    col_freq = jnp.arange(W, dtype=jnp.float32)
    lam = (4.0 * jnp.sin(jnp.pi * row_freq / TILE) ** 2)[:, None] + (4.0 * jnp.sin(jnp.pi * col_freq / W) ** 2)[None, :]
    filt = 1.0 / (1.0 + paganin_beta * lam)
    folded = jnp.minimum(col_freq, W - col_freq)
    ramp = ramp_gain * (folded / W) * (0.5 + 0.5 * jnp.cos(2.0 * jnp.pi * folded / W))

    def one_angle(angle_rows):
        tiles = angle_rows[row_index]
        spectrum = jnp.fft.fft2(tiles, axes=(1, 2)) * filt
        back = jnp.real(jnp.fft.ifft2(spectrum, axes=(1, 2)))
        paganin = back[:, HALO:HALO + RD, :].reshape(SLICES, W)
        filtered = jnp.real(jnp.fft.ifft(jnp.fft.fft(paganin, axis=-1) * ramp, axis=-1))
        return filtered.astype(jnp.bfloat16)

    sinogram = lax.map(one_angle, padded)
    offsets = jnp.arange(CB, dtype=jnp.int32)

    def one_region(region):
        starts = lax.dynamic_index_in_dim(block_start, region, 1, keepdims=False)
        index = (starts[:, None] + offsets[None, :]).astype(jnp.int32)
        index = jnp.broadcast_to(index[:, None, :], (ANGLES, SLICES, CB))
        blocks = jnp.take_along_axis(sinogram, index, axis=2)
        weights = lax.dynamic_slice_in_dim(bp_weights, region * PIX_DEV, PIX_DEV, 2)
        return jnp.einsum('asc,acp->sp', blocks.astype(jnp.float32), weights.astype(jnp.float32))

    parts = lax.map(one_region, jnp.arange(REGIONS, dtype=jnp.int32))
    return jnp.transpose(parts, (1, 0, 2)).reshape(SLICES, PIX)
```

```python
import functools

import jax
import jax.numpy as jnp
import numpy as np
from jax import lax
from jax.experimental import pallas as pl
from jax.experimental.pallas import tpu as pltpu
from jax.sharding import PartitionSpec as P

HALO = 4
LANES = 128
MESH = pl.DeviceIdType.MESH
paganin_beta = 8.0
ramp_gain = 320.0
NEAR = 4


def split(table):
    high = np.asarray(table, np.float32).astype(jnp.bfloat16)
    low = (np.asarray(table, np.float64) - high.astype(np.float64)).astype(np.float32).astype(jnp.bfloat16)
    return high, low


def tables(rows, width):
    blocks = width // LANES
    tile = rows + 2 * HALO
    half = blocks // 2
    t = np.arange(tile)
    basis, freqs = [np.full(tile, 1.0 / np.sqrt(tile))], [0]
    for u in range(1, tile // 2):
        basis += [np.sqrt(2.0 / tile) * np.cos(2 * np.pi * u * t / tile)]
        basis += [np.sqrt(2.0 / tile) * np.sin(2 * np.pi * u * t / tile)]
        freqs += [u, u]
    basis += [np.cos(np.pi * t) / np.sqrt(tile)]
    freqs += [tile // 2]
    basis, freqs = np.stack(basis), np.array(freqs)
    a, k = np.arange(blocks), np.arange(half + 1)
    turn = 2 * np.pi * np.outer(k, a) / blocks
    outer = np.concatenate([np.cos(turn), -np.sin(turn[1:half])])
    count = outer.shape[0] * tile

    def forward(cols):
        return np.einsum("ra,ut->ruat", outer, basis[:, cols]).reshape(count, -1)

    own = forward(slice(HALO, HALO + rows))
    halo = np.concatenate([forward(slice(0, HALO)), forward(slice(HALO + rows, tile))], axis=1)
    back = own.T
    b = np.arange(LANES)
    twist = 2 * np.pi * np.outer(k, b) / width
    wide = [np.repeat(x, 8, axis=0).astype(np.float32) for x in (np.cos(twist), np.sin(twist))]
    turn = 2 * np.pi * (np.outer(b, b) % LANES) / LANES
    c, s = np.cos(turn), np.sin(turn)
    inner = np.block([[c, -s], [s, c]])
    v = k[:, None] + blocks * b[None, :]
    lam = (4 * np.sin(np.pi * freqs / tile) ** 2)[None, :, None] + (4 * np.sin(np.pi * v / width) ** 2)[:, None, :]
    m = np.minimum(v, width - v)
    ramp = ramp_gain * (m / width) * (0.5 + 0.5 * np.cos(2 * np.pi * m / width))
    weight = np.where((k == 0) | (k == half), 1.0, 2.0)[:, None] / width
    gain = ((weight * ramp)[:, None, :] / (1 + paganin_beta * lam)).reshape(-1, LANES).astype(np.float32)
    own_h, own_l = split(own)
    halo_h, halo_l = split(halo)
    back_h, back_l = split(back)
    fore_h, fore_l = split(inner)
    hind_h, hind_l = split(inner.T)
    cat = functools.partial(np.concatenate, axis=1)
    return (
        cat([own_h, own_h, own_l]),
        cat([halo_h, halo_l]),
        np.stack(wide),
        np.stack([fore_h, fore_l]),
        gain,
        np.stack([hind_h, hind_l]),
        cat([back_h, back_h, back_l]),
    )


def halves(x):
    high = x.astype(jnp.bfloat16)
    return high, (x - high.astype(jnp.float32)).astype(jnp.bfloat16)


def dot(x, y):
    return jnp.dot(x, y, preferred_element_type=jnp.float32)


def data_times(x, table):
    high, low = halves(x)
    return dot(high, table[0]) + dot(low, table[0]) + dot(high, table[1])


def table_times(table, x):
    high, low = halves(x)
    return dot(table, jnp.concatenate([high, low, high], axis=0))


def block_transpose(x, group, pair):
    out = x
    for d in range(1, 4):
        moved = pltpu.roll(pltpu.roll(x, 32 * d, 1), 8 - 2 * d, 0)
        out = jnp.where((group - pair) % 4 == d, moved, out)
    return out


def kernel(
    peers,
    proj_hbm,
    flat_hbm,
    start_hbm,
    own_hbm,
    halo_hbm,
    wide_hbm,
    fore_hbm,
    gain_hbm,
    hind_hbm,
    back_hbm,
    out_ref,
    proj,
    flat,
    starts,
    own_t,
    halo_t,
    wide,
    fore,
    gain,
    hind,
    back,
    edge,
    halo,
    sino,
    send,
    recv,
    load_sem,
    edge_sem,
    halo_sem,
    send_sem,
    recv_sem,
    round_sem,
):
    me = lax.axis_index("ang")
    row = lax.axis_index("row")
    row_count = lax.axis_size("row")
    rows, width = flat.shape
    blocks = width // LANES
    half = blocks // 2
    tile = rows + 2 * HALO

    def peer(d):
        return {"ang": lax.rem(me + (d + peers), peers)}

    def signal(sem, device):
        pl.semaphore_signal(sem, inc=1, device_id=device, device_id_type=MESH)

    barrier = pltpu.get_barrier_semaphore()
    for d in range(1, NEAR + 1):
        signal(barrier, peer(d))
        signal(barrier, peer(-d))

    @pl.when(row > 0)
    def _():
        signal(barrier, {"row": row - 1})

    @pl.when(row < row_count - 1)
    def _():
        signal(barrier, {"row": row + 1})

    loads = [
        pltpu.make_async_copy(src, dst, load_sem.at[i])
        for i, (src, dst) in enumerate(
            [
                (proj_hbm, proj),
                (flat_hbm, flat),
                (own_hbm, own_t),
                (halo_hbm, halo_t),
                (wide_hbm, wide),
                (fore_hbm, fore),
                (gain_hbm, gain),
                (hind_hbm, hind),
                (back_hbm, back),
                (start_hbm, starts),
            ]
        )
    ]
    for load in loads:
        load.start()

    sub = lax.broadcasted_iota(jnp.int32, (8, LANES), 0)
    lane = lax.broadcasted_iota(jnp.int32, (8, LANES), 1)
    loads[0].wait()
    loads[1].wait()
    contrast = []
    for a in range(blocks):
        cols = slice(a * LANES, (a + 1) * LANES)
        contrast.append(1.0 - proj[0, :, cols].astype(jnp.float32) / flat[:, cols])
    for a in range(0, blocks, 4):
        first, last = [], []
        for i in (a, a + 2):
            x, y = contrast[i], contrast[i + 1]
            first.append(jnp.where(sub < HALO, x, pltpu.roll(y, HALO, 0)))
            last.append(jnp.where(sub < HALO, pltpu.roll(x, HALO, 0), y))
        edge[0, a * HALO : (a + 4) * HALO, :] = jnp.concatenate(first, axis=0).astype(jnp.bfloat16)
        edge[1, a * HALO : (a + 4) * HALO, :] = jnp.concatenate(last, axis=0).astype(jnp.bfloat16)

    near = 2 * NEAR

    @pl.when((row > 0) & (row < row_count - 1))
    def _():
        pl.semaphore_wait(barrier, near + 2)

    @pl.when((row == 0) | (row == row_count - 1))
    def _():
        pl.semaphore_wait(barrier, near + 1)

    def edge_copy(which, to):
        return pltpu.make_async_remote_copy(
            src_ref=edge.at[which],
            dst_ref=halo.at[1 - which],
            send_sem=edge_sem.at[which],
            recv_sem=halo_sem.at[1 - which],
            device_id={"row": to},
            device_id_type=MESH,
        )

    up, down = edge_copy(0, row - 1), edge_copy(1, row + 1)

    @pl.when(row > 0)
    def _():
        up.start()

    @pl.when(row < row_count - 1)
    def _():
        down.start()

    signal(round_sem.at[0], peer(NEAR))
    signal(round_sem.at[0], peer(-NEAR))

    @pl.when(row == 0)
    def _():
        halo[0] = jnp.zeros(halo.shape[1:], halo.dtype)

    @pl.when(row == row_count - 1)
    def _():
        halo[1] = jnp.zeros(halo.shape[1:], halo.dtype)

    loads[2].wait()
    spread = table_times(own_t[...], jnp.concatenate(contrast, axis=0))

    pl.semaphore_wait(round_sem.at[0], 2)
    signal(round_sem.at[1], peer(2 * NEAR))
    signal(round_sem.at[1], peer(-2 * NEAR))

    for load in loads[3:]:
        load.wait()

    @pl.when(row > 0)
    def _():
        up.wait_send()
        pltpu.make_async_copy(halo.at[0], halo.at[0], halo_sem.at[0]).wait()

    @pl.when(row < row_count - 1)
    def _():
        down.wait_send()
        pltpu.make_async_copy(halo.at[1], halo.at[1], halo_sem.at[1]).wait()

    sides = jnp.concatenate([halo[0], halo[1]], axis=0)
    spread = spread + dot(halo_t[...], jnp.concatenate([sides, sides], axis=0))

    turn_re, turn_im = [], []
    for k in range(half + 1):
        c, s = wide[0, 8 * k : 8 * k + 8], wide[1, 8 * k : 8 * k + 8]
        for j in range(0, tile, 8):
            re = spread[tile * k + j : tile * k + j + 8]
            if 0 < k < half:
                spot = tile * (half + k) + j
                im = spread[spot : spot + 8]
                turn_re.append(re * c + im * s)
                turn_im.append(im * c - re * s)
            else:
                turn_re.append(re * c)
                turn_im.append(-(re * s))
    turned = jnp.concatenate([jnp.concatenate(turn_re, axis=0), jnp.concatenate(turn_im, axis=0)], axis=1)
    spectrum = data_times(turned, fore)
    scale = gain[...]
    spectrum = spectrum * jnp.concatenate([scale, scale], axis=1)
    undone = data_times(spectrum, hind)
    real, imag = [], []
    for k in range(half + 1):
        c, s = wide[0, 8 * k : 8 * k + 8], wide[1, 8 * k : 8 * k + 8]
        for j in range(0, tile, 8):
            re = undone[tile * k + j : tile * k + j + 8, :LANES]
            im = undone[tile * k + j : tile * k + j + 8, LANES:]
            real.append(re * c - im * s)
            if 0 < k < half:
                imag.append(im * c + re * s)
    filtered = table_times(back[...], jnp.concatenate(real + imag, axis=0))
    for a in range(blocks):
        sino[a] = filtered[8 * a : 8 * a + 8]

    group, pair = lane // 32, sub // 2
    for j in range(0, peers, 4):
        merged = None
        for q in range(4):
            begin = starts[me, j + q]
            a, b = begin // LANES, begin % LANES
            piece = jnp.where(lane >= b, sino[a], sino[jnp.minimum(a + 1, blocks - 1)])
            piece = pltpu.roll(piece, lax.rem(32 * q - b + LANES, LANES), 1)
            merged = piece if q == 0 else jnp.where(group == q, piece, merged)
        packed = block_transpose(merged, group, pair)
        for q in range(4):
            send[j + q] = packed[2 * q : 2 * q + 2].astype(jnp.bfloat16)

    pl.semaphore_wait(round_sem.at[1], 2)
    order = sorted(range(1, peers), key=lambda d: -min(d, peers - d))
    for d in order:
        to = lax.rem(me + d, peers)
        pltpu.make_async_remote_copy(
            src_ref=send.at[to],
            dst_ref=recv.at[me],
            send_sem=send_sem,
            recv_sem=recv_sem,
            device_id={"ang": to},
            device_id_type=MESH,
        ).start()
    recv[me] = send[me]
    some = recv.at[pl.ds(0, peers - 1)]
    pltpu.make_async_copy(some, some, recv_sem).wait()
    for j in range(0, peers, 4):
        packed = jnp.concatenate([recv[j + q].astype(jnp.float32) for q in range(4)], axis=0)
        out_ref[:, j * 32 : (j + 4) * 32] = block_transpose(packed, group, pair).astype(jnp.bfloat16)
    some = send.at[pl.ds(0, peers - 1)]
    pltpu.make_async_copy(some, some, send_sem).wait()


def body(projections, flats, block_start, bp_weights):
    rows, width = flats.shape
    peers = lax.axis_size("ang")
    columns = bp_weights.shape[1]
    consts = [jnp.asarray(x) for x in tables(rows, width)]
    operands = [projections, flats, block_start, *consts]
    blocks = width // LANES
    hbm = pl.BlockSpec(memory_space=pl.ANY)
    gathered = pl.pallas_call(
        functools.partial(kernel, peers),
        out_shape=jax.ShapeDtypeStruct((rows, peers * columns), jnp.bfloat16),
        in_specs=[hbm] * len(operands),
        out_specs=pl.BlockSpec(memory_space=pltpu.VMEM),
        scratch_shapes=[
            pltpu.VMEM(projections.shape, projections.dtype),
            pltpu.VMEM(flats.shape, flats.dtype),
            pltpu.SMEM(block_start.shape, block_start.dtype),
            *[pltpu.VMEM(x.shape, x.dtype) for x in consts],
            pltpu.VMEM((2, blocks * HALO, LANES), jnp.bfloat16),
            pltpu.VMEM((2, blocks * HALO, LANES), jnp.bfloat16),
            pltpu.VMEM((blocks, rows, LANES), jnp.float32),
            pltpu.VMEM((peers, 2, LANES), jnp.bfloat16),
            pltpu.VMEM((peers, 2, LANES), jnp.bfloat16),
            pltpu.SemaphoreType.DMA((len(operands),)),
            pltpu.SemaphoreType.DMA((2,)),
            pltpu.SemaphoreType.DMA((2,)),
            pltpu.SemaphoreType.DMA,
            pltpu.SemaphoreType.DMA,
            pltpu.SemaphoreType.REGULAR((2,)),
        ],
        compiler_params=pltpu.CompilerParams(collective_id=0, has_side_effects=True),
    )(*operands)
    weights = bp_weights.reshape(-1, bp_weights.shape[2])
    return lax.dot_general(gathered, weights, (((1,), (0,)), ((), ())), preferred_element_type=jnp.float32)


def solution(mesh):
    placed = (P(("scan", "ang"), "row", None), P(("scan", "row"), None), P(), P(None, None, "ang"))
    return jax.shard_map(
        body, mesh=mesh, in_specs=placed, out_specs=P(("scan", "row"), "ang"), check_vma=False
    )
```

```python
import functools

import jax
import jax.numpy as jnp
import numpy as np
from jax import lax
from jax.experimental import pallas as pl
from jax.experimental.pallas import tpu as pltpu
from jax.sharding import PartitionSpec as P

HALO = 4
LANES = 128
MESH = pl.DeviceIdType.MESH
paganin_beta = 8.0
ramp_gain = 320.0
NEAR = 4


def split(table):
    high = np.asarray(table, np.float32).astype(jnp.bfloat16)
    low = (np.asarray(table, np.float64) - high.astype(np.float64)).astype(np.float32).astype(jnp.bfloat16)
    return high, low


def tables(rows, width):
    blocks = width // LANES
    tile = rows + 2 * HALO
    half = blocks // 2
    t = np.arange(tile)
    basis, freqs = [np.full(tile, 1.0 / np.sqrt(tile))], [0]
    for u in range(1, tile // 2):
        basis += [np.sqrt(2.0 / tile) * np.cos(2 * np.pi * u * t / tile)]
        basis += [np.sqrt(2.0 / tile) * np.sin(2 * np.pi * u * t / tile)]
        freqs += [u, u]
    basis += [np.cos(np.pi * t) / np.sqrt(tile)]
    freqs += [tile // 2]
    basis, freqs = np.stack(basis), np.array(freqs)
    a, k = np.arange(blocks), np.arange(half + 1)
    turn = 2 * np.pi * np.outer(k, a) / blocks
    outer = np.concatenate([np.cos(turn), -np.sin(turn[1:half])])
    count = outer.shape[0] * tile

    def forward(cols):
        return np.einsum("ra,ut->ruat", outer, basis[:, cols]).reshape(count, -1)

    own = forward(slice(HALO, HALO + rows))
    halo = np.concatenate([forward(slice(0, HALO)), forward(slice(HALO + rows, tile))], axis=1)
    back = own.T
    b = np.arange(LANES)
    twist = 2 * np.pi * np.outer(k, b) / width
    wide = [np.repeat(x, 8, axis=0).astype(np.float32) for x in (np.cos(twist), np.sin(twist))]
    turn = 2 * np.pi * (np.outer(b, b) % LANES) / LANES
    c, s = np.cos(turn), np.sin(turn)
    inner = np.block([[c, -s], [s, c]])
    v = k[:, None] + blocks * b[None, :]
    lam = (4 * np.sin(np.pi * freqs / tile) ** 2)[None, :, None] + (4 * np.sin(np.pi * v / width) ** 2)[:, None, :]
    m = np.minimum(v, width - v)
    ramp = ramp_gain * (m / width) * (0.5 + 0.5 * np.cos(2 * np.pi * m / width))
    weight = np.where((k == 0) | (k == half), 1.0, 2.0)[:, None] / width
    gain = ((weight * ramp)[:, None, :] / (1 + paganin_beta * lam)).reshape(-1, LANES).astype(np.float32)
    own_h, own_l = split(own)
    halo_h, halo_l = split(halo)
    back_h, back_l = split(back)
    fore_h, fore_l = split(inner)
    hind_h, hind_l = split(inner.T)
    cat = functools.partial(np.concatenate, axis=1)
    return (
        cat([own_h, own_h, own_l]),
        cat([halo_h, halo_l]),
        np.stack(wide),
        np.stack([fore_h, fore_l]),
        gain,
        np.stack([hind_h, hind_l]),
        cat([back_h, back_h, back_l]),
    )


def halves(x):
    high = x.astype(jnp.bfloat16)
    return high, (x - high.astype(jnp.float32)).astype(jnp.bfloat16)


def dot(x, y):
    return jnp.dot(x, y, preferred_element_type=jnp.float32)


def data_times(x, table):
    high, low = halves(x)
    return dot(high, table[0]) + dot(low, table[0]) + dot(high, table[1])


def table_times(table, x):
    high, low = halves(x)
    return dot(table, jnp.concatenate([high, low, high], axis=0))


def block_transpose(x, group, pair):
    out = x
    for d in range(1, 4):
        moved = pltpu.roll(pltpu.roll(x, 32 * d, 1), 8 - 2 * d, 0)
        out = jnp.where((group - pair) % 4 == d, moved, out)
    return out


def kernel(
    peers,
    proj_hbm,
    flat_hbm,
    start_hbm,
    own_hbm,
    halo_hbm,
    wide_hbm,
    fore_hbm,
    gain_hbm,
    hind_hbm,
    back_hbm,
    weights_hbm,
    out_ref,
    proj,
    flat,
    starts,
    own_t,
    halo_t,
    wide,
    fore,
    gain,
    hind,
    back,
    weights,
    edge,
    halo,
    sino,
    send,
    recv,
    load_sem,
    edge_sem,
    halo_sem,
    send_sem,
    recv_sem,
    round_sem,
):
    me = lax.axis_index("ang")
    row = lax.axis_index("row")
    row_count = lax.axis_size("row")
    rows, width = flat.shape
    blocks = width // LANES
    half = blocks // 2
    tile = rows + 2 * HALO

    def peer(d):
        return {"ang": lax.rem(me + (d + peers), peers)}

    def signal(sem, device):
        pl.semaphore_signal(sem, inc=1, device_id=device, device_id_type=MESH)

    barrier = pltpu.get_barrier_semaphore()
    for d in range(1, NEAR + 1):
        signal(barrier, peer(d))
        signal(barrier, peer(-d))

    @pl.when(row > 0)
    def _():
        signal(barrier, {"row": row - 1})

    @pl.when(row < row_count - 1)
    def _():
        signal(barrier, {"row": row + 1})

    loads = [
        pltpu.make_async_copy(src, dst, load_sem.at[i])
        for i, (src, dst) in enumerate(
            [
                (proj_hbm, proj),
                (flat_hbm, flat),
                (own_hbm, own_t),
                (halo_hbm, halo_t),
                (wide_hbm, wide),
                (fore_hbm, fore),
                (gain_hbm, gain),
                (hind_hbm, hind),
                (back_hbm, back),
                (start_hbm, starts),
                (weights_hbm, weights),
            ]
        )
    ]
    for load in loads:
        load.start()

    sub = lax.broadcasted_iota(jnp.int32, (8, LANES), 0)
    lane = lax.broadcasted_iota(jnp.int32, (8, LANES), 1)
    loads[0].wait()
    loads[1].wait()
    contrast = []
    for a in range(blocks):
        cols = slice(a * LANES, (a + 1) * LANES)
        contrast.append(1.0 - proj[0, :, cols].astype(jnp.float32) / flat[:, cols])
    for a in range(0, blocks, 4):
        first, last = [], []
        for i in (a, a + 2):
            x, y = contrast[i], contrast[i + 1]
            first.append(jnp.where(sub < HALO, x, pltpu.roll(y, HALO, 0)))
            last.append(jnp.where(sub < HALO, pltpu.roll(x, HALO, 0), y))
        edge[0, a * HALO : (a + 4) * HALO, :] = jnp.concatenate(first, axis=0).astype(jnp.bfloat16)
        edge[1, a * HALO : (a + 4) * HALO, :] = jnp.concatenate(last, axis=0).astype(jnp.bfloat16)

    near = 2 * NEAR

    @pl.when((row > 0) & (row < row_count - 1))
    def _():
        pl.semaphore_wait(barrier, near + 2)

    @pl.when((row == 0) | (row == row_count - 1))
    def _():
        pl.semaphore_wait(barrier, near + 1)

    def edge_copy(which, to):
        return pltpu.make_async_remote_copy(
            src_ref=edge.at[which],
            dst_ref=halo.at[1 - which],
            send_sem=edge_sem.at[which],
            recv_sem=halo_sem.at[1 - which],
            device_id={"row": to},
            device_id_type=MESH,
        )

    up, down = edge_copy(0, row - 1), edge_copy(1, row + 1)

    @pl.when(row > 0)
    def _():
        up.start()

    @pl.when(row < row_count - 1)
    def _():
        down.start()

    signal(round_sem.at[0], peer(NEAR))
    signal(round_sem.at[0], peer(-NEAR))

    @pl.when(row == 0)
    def _():
        halo[0] = jnp.zeros(halo.shape[1:], halo.dtype)

    @pl.when(row == row_count - 1)
    def _():
        halo[1] = jnp.zeros(halo.shape[1:], halo.dtype)

    loads[2].wait()
    spread = table_times(own_t[...], jnp.concatenate(contrast, axis=0))

    pl.semaphore_wait(round_sem.at[0], 2)
    signal(round_sem.at[1], peer(2 * NEAR))
    signal(round_sem.at[1], peer(-2 * NEAR))

    for load in loads[3:-1]:
        load.wait()

    @pl.when(row > 0)
    def _():
        up.wait_send()
        pltpu.make_async_copy(halo.at[0], halo.at[0], halo_sem.at[0]).wait()

    @pl.when(row < row_count - 1)
    def _():
        down.wait_send()
        pltpu.make_async_copy(halo.at[1], halo.at[1], halo_sem.at[1]).wait()

    sides = jnp.concatenate([halo[0], halo[1]], axis=0)
    spread = spread + dot(halo_t[...], jnp.concatenate([sides, sides], axis=0))

    turn_re, turn_im = [], []
    for k in range(half + 1):
        c, s = wide[0, 8 * k : 8 * k + 8], wide[1, 8 * k : 8 * k + 8]
        for j in range(0, tile, 8):
            re = spread[tile * k + j : tile * k + j + 8]
            if 0 < k < half:
                spot = tile * (half + k) + j
                im = spread[spot : spot + 8]
                turn_re.append(re * c + im * s)
                turn_im.append(im * c - re * s)
            else:
                turn_re.append(re * c)
                turn_im.append(-(re * s))
    turned = jnp.concatenate([jnp.concatenate(turn_re, axis=0), jnp.concatenate(turn_im, axis=0)], axis=1)
    spectrum = data_times(turned, fore)
    scale = gain[...]
    spectrum = spectrum * jnp.concatenate([scale, scale], axis=1)
    undone = data_times(spectrum, hind)
    real, imag = [], []
    for k in range(half + 1):
        c, s = wide[0, 8 * k : 8 * k + 8], wide[1, 8 * k : 8 * k + 8]
        for j in range(0, tile, 8):
            re = undone[tile * k + j : tile * k + j + 8, :LANES]
            im = undone[tile * k + j : tile * k + j + 8, LANES:]
            real.append(re * c - im * s)
            if 0 < k < half:
                imag.append(im * c + re * s)
    filtered = table_times(back[...], jnp.concatenate(real + imag, axis=0))
    for a in range(blocks):
        sino[a] = filtered[8 * a : 8 * a + 8]

    group, pair = lane // 32, sub // 2
    for j in range(0, peers, 4):
        merged = None
        for q in range(4):
            begin = starts[me, j + q]
            a, b = begin // LANES, begin % LANES
            piece = jnp.where(lane >= b, sino[a], sino[jnp.minimum(a + 1, blocks - 1)])
            piece = pltpu.roll(piece, lax.rem(32 * q - b + LANES, LANES), 1)
            merged = piece if q == 0 else jnp.where(group == q, piece, merged)
        packed = block_transpose(merged, group, pair)
        for q in range(4):
            send[j + q] = packed[2 * q : 2 * q + 2].astype(jnp.bfloat16)

    pl.semaphore_wait(round_sem.at[1], 2)
    order = sorted(range(1, peers), key=lambda d: -min(d, peers - d))
    for d in order:
        to = lax.rem(me + d, peers)
        pltpu.make_async_remote_copy(
            src_ref=send.at[to],
            dst_ref=recv.at[me],
            send_sem=send_sem,
            recv_sem=recv_sem,
            device_id={"ang": to},
            device_id_type=MESH,
        ).start()
    recv[me] = send[me]
    some = recv.at[pl.ds(0, peers - 1)]
    pltpu.make_async_copy(some, some, recv_sem).wait()
    loads[-1].wait()
    blocks_in = []
    for j in range(0, peers, 4):
        packed = jnp.concatenate([recv[j + q].astype(jnp.float32) for q in range(4)], axis=0)
        blocks_in.append(block_transpose(packed, group, pair).astype(jnp.bfloat16))
    out_ref[...] = dot(jnp.concatenate(blocks_in, axis=1), weights[...])
    some = send.at[pl.ds(0, peers - 1)]
    pltpu.make_async_copy(some, some, send_sem).wait()


def body(projections, flats, block_start, bp_weights):
    rows, width = flats.shape
    peers = lax.axis_size("ang")
    weights = bp_weights.reshape(-1, bp_weights.shape[2])
    consts = [jnp.asarray(x) for x in tables(rows, width)]
    operands = [projections, flats, block_start, *consts, weights]
    blocks = width // LANES
    hbm = pl.BlockSpec(memory_space=pl.ANY)
    return pl.pallas_call(
        functools.partial(kernel, peers),
        out_shape=pltpu.VMEM((rows, weights.shape[1]), jnp.float32),
        in_specs=[hbm] * len(operands),
        out_specs=pl.BlockSpec(memory_space=pltpu.VMEM),
        scratch_shapes=[
            pltpu.VMEM(projections.shape, projections.dtype),
            pltpu.VMEM(flats.shape, flats.dtype),
            pltpu.SMEM(block_start.shape, block_start.dtype),
            *[pltpu.VMEM(x.shape, x.dtype) for x in (*consts, weights)],
            pltpu.VMEM((2, blocks * HALO, LANES), jnp.bfloat16),
            pltpu.VMEM((2, blocks * HALO, LANES), jnp.bfloat16),
            pltpu.VMEM((blocks, rows, LANES), jnp.float32),
            pltpu.VMEM((peers, 2, LANES), jnp.bfloat16),
            pltpu.VMEM((peers, 2, LANES), jnp.bfloat16),
            pltpu.SemaphoreType.DMA((len(operands),)),
            pltpu.SemaphoreType.DMA((2,)),
            pltpu.SemaphoreType.DMA((2,)),
            pltpu.SemaphoreType.DMA,
            pltpu.SemaphoreType.DMA,
            pltpu.SemaphoreType.REGULAR((2,)),
        ],
        compiler_params=pltpu.CompilerParams(collective_id=0, has_side_effects=True),
    )(*operands)


def solution(mesh):
    placed = (P(("scan", "ang"), "row", None), P(("scan", "row"), None), P(), P(None, None, "ang"))
    return jax.shard_map(
        body, mesh=mesh, in_specs=placed, out_specs=P(("scan", "row"), "ang"), check_vma=False
    )
```

```python
import functools

import jax
import jax.numpy as jnp
import numpy as np
from jax import lax
from jax.experimental import pallas as pl
from jax.experimental.pallas import tpu as pltpu
from jax.sharding import PartitionSpec as P

HALO = 4
LANES = 128
MESH = pl.DeviceIdType.MESH
paganin_beta = 8.0
ramp_gain = 320.0
NEAR = 2


def split(table):
    high = np.asarray(table, np.float32).astype(jnp.bfloat16)
    low = (np.asarray(table, np.float64) - high.astype(np.float64)).astype(np.float32).astype(jnp.bfloat16)
    return high, low


def tables(rows, width):
    blocks = width // LANES
    tile = rows + 2 * HALO
    half = blocks // 2
    t = np.arange(tile)
    basis, freqs = [np.full(tile, 1.0 / np.sqrt(tile))], [0]
    for u in range(1, tile // 2):
        basis += [np.sqrt(2.0 / tile) * np.cos(2 * np.pi * u * t / tile)]
        basis += [np.sqrt(2.0 / tile) * np.sin(2 * np.pi * u * t / tile)]
        freqs += [u, u]
    basis += [np.cos(np.pi * t) / np.sqrt(tile)]
    freqs += [tile // 2]
    basis, freqs = np.stack(basis), np.array(freqs)
    a, k = np.arange(blocks), np.arange(half + 1)
    turn = 2 * np.pi * np.outer(k, a) / blocks
    outer = np.concatenate([np.cos(turn), -np.sin(turn[1:half])])
    count = outer.shape[0] * tile

    def forward(cols):
        return np.einsum("ra,ut->ruat", outer, basis[:, cols]).reshape(count, -1)

    own = forward(slice(HALO, HALO + rows))
    halo = np.concatenate([forward(slice(0, HALO)), forward(slice(HALO + rows, tile))], axis=1)
    back = own.T
    b = np.arange(LANES)
    twist = 2 * np.pi * np.outer(k, b) / width
    wide = [np.repeat(x, 8, axis=0).astype(np.float32) for x in (np.cos(twist), np.sin(twist))]
    turn = 2 * np.pi * (np.outer(b, b) % LANES) / LANES
    c, s = np.cos(turn), np.sin(turn)
    inner = np.block([[c, -s], [s, c]])
    v = k[:, None] + blocks * b[None, :]
    lam = (4 * np.sin(np.pi * freqs / tile) ** 2)[None, :, None] + (4 * np.sin(np.pi * v / width) ** 2)[:, None, :]
    m = np.minimum(v, width - v)
    ramp = ramp_gain * (m / width) * (0.5 + 0.5 * np.cos(2 * np.pi * m / width))
    weight = np.where((k == 0) | (k == half), 1.0, 2.0)[:, None] / width
    gain = ((weight * ramp)[:, None, :] / (1 + paganin_beta * lam)).reshape(-1, LANES).astype(np.float32)
    own_h, own_l = split(own)
    halo_h, halo_l = split(halo)
    back_h, back_l = split(back)
    fore_h, fore_l = split(inner)
    hind_h, hind_l = split(inner.T)
    cat = functools.partial(np.concatenate, axis=1)
    return (
        cat([own_h, own_h, own_l]),
        cat([halo_h, halo_l]),
        np.stack(wide),
        np.stack([fore_h, fore_l]),
        gain,
        np.stack([hind_h, hind_l]),
        cat([back_h, back_h, back_l]),
    )


def halves(x):
    high = x.astype(jnp.bfloat16)
    return high, (x - high.astype(jnp.float32)).astype(jnp.bfloat16)


def dot(x, y):
    return jnp.dot(x, y, preferred_element_type=jnp.float32)


def data_times(x, table):
    high, low = halves(x)
    return dot(high, table[0]) + dot(low, table[0]) + dot(high, table[1])


def table_times(table, x):
    high, low = halves(x)
    return dot(table, jnp.concatenate([high, low, high], axis=0))


def block_transpose(x, group, pair):
    out = x
    for d in range(1, 4):
        moved = pltpu.roll(pltpu.roll(x, 32 * d, 1), 8 - 2 * d, 0)
        out = jnp.where((group - pair) % 4 == d, moved, out)
    return out


def kernel(
    peers,
    proj_hbm,
    flat_hbm,
    start_hbm,
    own_hbm,
    halo_hbm,
    wide_hbm,
    fore_hbm,
    gain_hbm,
    hind_hbm,
    back_hbm,
    weights_hbm,
    out_ref,
    proj,
    flat,
    starts,
    own_t,
    halo_t,
    wide,
    fore,
    gain,
    hind,
    back,
    weights,
    spread,
    edge,
    halo,
    sino,
    send,
    recv,
    relay_up,
    relay_down,
    load_sem,
    edge_sem,
    halo_sem,
    send_sem,
    recv_sem,
    relay_sem,
    bundle_send_sem,
    bundle_sem,
    round_sem,
):
    me = lax.axis_index("ang")
    row = lax.axis_index("row")
    row_count = lax.axis_size("row")
    rows, width = flat.shape
    blocks = width // LANES
    half = blocks // 2
    tile = rows + 2 * HALO

    def peer(d):
        return {"ang": lax.rem(me + (d + peers), peers)}

    def signal(sem, device):
        pl.semaphore_signal(sem, inc=1, device_id=device, device_id_type=MESH)

    loads = [
        pltpu.make_async_copy(src, dst, load_sem.at[i])
        for i, (src, dst) in enumerate(
            [
                (proj_hbm, proj),
                (flat_hbm, flat),
                (own_hbm, own_t),
                (halo_hbm, halo_t),
                (wide_hbm, wide),
                (fore_hbm, fore),
                (gain_hbm, gain),
                (hind_hbm, hind),
                (back_hbm, back),
                (start_hbm, starts),
                (weights_hbm, weights),
            ]
        )
    ]
    for load in loads[:2]:
        load.start()

    barrier = pltpu.get_barrier_semaphore()
    for d in range(1, NEAR + 1):
        signal(barrier, peer(d))
        signal(barrier, peer(-d))

    @pl.when(row > 0)
    def _():
        signal(barrier, {"row": row - 1})

    @pl.when(row < row_count - 1)
    def _():
        signal(barrier, {"row": row + 1})

    for load in loads[2:]:
        load.start()

    near = 2 * NEAR

    @pl.when((row > 0) & (row < row_count - 1))
    def _():
        pl.semaphore_wait(barrier, near + 2)

    @pl.when((row == 0) | (row == row_count - 1))
    def _():
        pl.semaphore_wait(barrier, near + 1)

    signal(round_sem.at[0], peer(NEAR))
    signal(round_sem.at[0], peer(-NEAR))

    sub = lax.broadcasted_iota(jnp.int32, (8, LANES), 0)
    lane = lax.broadcasted_iota(jnp.int32, (8, LANES), 1)
    loads[0].wait()
    loads[1].wait()
    contrast = []
    for a in range(blocks):
        cols = slice(a * LANES, (a + 1) * LANES)
        contrast.append(1.0 - proj[0, :, cols].astype(jnp.float32) / flat[:, cols])
    for a in range(0, blocks, 4):
        first, last = [], []
        for i in (a, a + 2):
            x, y = contrast[i], contrast[i + 1]
            first.append(jnp.where(sub < HALO, x, pltpu.roll(y, HALO, 0)))
            last.append(jnp.where(sub < HALO, pltpu.roll(x, HALO, 0), y))
        edge[0, a * HALO : (a + 4) * HALO, :] = jnp.concatenate(first, axis=0).astype(jnp.bfloat16)
        edge[1, a * HALO : (a + 4) * HALO, :] = jnp.concatenate(last, axis=0).astype(jnp.bfloat16)

    def edge_copy(which, to):
        return pltpu.make_async_remote_copy(
            src_ref=edge.at[which],
            dst_ref=halo.at[1 - which],
            send_sem=edge_sem.at[which],
            recv_sem=halo_sem.at[1 - which],
            device_id={"row": to},
            device_id_type=MESH,
        )

    up, down = edge_copy(0, row - 1), edge_copy(1, row + 1)

    @pl.when(row > 0)
    def _():
        up.start()

    @pl.when(row < row_count - 1)
    def _():
        down.start()

    @pl.when(row == 0)
    def _():
        halo[0] = jnp.zeros(halo.shape[1:], halo.dtype)

    @pl.when(row == row_count - 1)
    def _():
        halo[1] = jnp.zeros(halo.shape[1:], halo.dtype)

    loads[2].wait()
    spread[...] = table_times(own_t[...], jnp.concatenate(contrast, axis=0))

    pl.semaphore_wait(round_sem.at[0], 2)
    signal(round_sem.at[1], peer(2 * NEAR))
    signal(round_sem.at[1], peer(-2 * NEAR))

    for load in loads[3:-1]:
        load.wait()

    @pl.when(row > 0)
    def _():
        up.wait_send()
        pltpu.make_async_copy(halo.at[0], halo.at[0], halo_sem.at[0]).wait()

    @pl.when(row < row_count - 1)
    def _():
        down.wait_send()
        pltpu.make_async_copy(halo.at[1], halo.at[1], halo_sem.at[1]).wait()

    sides = jnp.concatenate([halo[0], halo[1]], axis=0)
    first = spread[...] + dot(halo_t[...], jnp.concatenate([sides, sides], axis=0))

    turn_re, turn_im = [], []
    for k in range(half + 1):
        c, s = wide[0, 8 * k : 8 * k + 8], wide[1, 8 * k : 8 * k + 8]
        for j in range(0, tile, 8):
            re = first[tile * k + j : tile * k + j + 8]
            if 0 < k < half:
                spot = tile * (half + k) + j
                im = first[spot : spot + 8]
                turn_re.append(re * c + im * s)
                turn_im.append(im * c - re * s)
            else:
                turn_re.append(re * c)
                turn_im.append(-(re * s))
    turned = jnp.concatenate([jnp.concatenate(turn_re, axis=0), jnp.concatenate(turn_im, axis=0)], axis=1)
    spectrum = data_times(turned, fore)
    scale = gain[...]
    spectrum = spectrum * jnp.concatenate([scale, scale], axis=1)
    undone = data_times(spectrum, hind)
    real, imag = [], []
    for k in range(half + 1):
        c, s = wide[0, 8 * k : 8 * k + 8], wide[1, 8 * k : 8 * k + 8]
        for j in range(0, tile, 8):
            re = undone[tile * k + j : tile * k + j + 8, :LANES]
            im = undone[tile * k + j : tile * k + j + 8, LANES:]
            real.append(re * c - im * s)
            if 0 < k < half:
                imag.append(im * c + re * s)
    filtered = table_times(back[...], jnp.concatenate(real + imag, axis=0))
    for a in range(blocks):
        sino[a] = filtered[8 * a : 8 * a + 8]

    group, pair = lane // 32, sub // 2
    for j in range(0, peers, 4):
        merged = None
        for q in range(4):
            begin = starts[me, j + q]
            a, b = begin // LANES, begin % LANES
            piece = jnp.where(lane >= b, sino[a], sino[jnp.minimum(a + 1, blocks - 1)])
            piece = pltpu.roll(piece, lax.rem(32 * q - b + LANES, LANES), 1)
            merged = piece if q == 0 else jnp.where(group == q, piece, merged)
        packed = block_transpose(merged, group, pair)
        for q in range(4):
            send[j + q] = packed[2 * q : 2 * q + 2].astype(jnp.bfloat16)

    far = peers // 4

    def hand(block, to, slot, sem):
        pltpu.make_async_remote_copy(
            src_ref=send.at[lax.rem(me + block + peers, peers)],
            dst_ref=slot,
            send_sem=send_sem,
            recv_sem=sem,
            device_id=peer(to),
            device_id_type=MESH,
        ).start()

    for d in range(1, far + 1):
        if d == 2 * NEAR + 1:
            pl.semaphore_wait(round_sem.at[1], 2)
        hand(d, d, recv.at[peers - d], recv_sem)
        hand(-d, -d, recv.at[d], recv_sem)
        hand(d + far, d, relay_up.at[far - d], relay_sem.at[0])
        if d < far:
            hand(-d - far, -d, relay_down.at[d - 1], relay_sem.at[1])
    recv[0] = send[me]

    def wait(ref, sem):
        pltpu.make_async_copy(ref, ref, sem).wait()

    def bundle(which, to, source, spots):
        return pltpu.make_async_remote_copy(
            src_ref=source,
            dst_ref=recv.at[spots],
            send_sem=bundle_send_sem.at[which],
            recv_sem=bundle_sem.at[which],
            device_id=peer(to),
            device_id_type=MESH,
        )

    up_bundle = bundle(0, far, relay_up, pl.ds(peers - 2 * far, far))
    down_bundle = bundle(1, -far, relay_down, pl.ds(far + 1, far - 1))
    wait(relay_up, relay_sem.at[0])
    up_bundle.start()
    wait(relay_down, relay_sem.at[1])
    down_bundle.start()
    wait(recv.at[pl.ds(0, 2 * far)], recv_sem)
    up_bundle.wait_recv()
    down_bundle.wait_recv()
    loads[-1].wait()
    blocks_in = []
    for j in range(0, peers, 4):
        spots = [lax.rem(j + q + peers - me, peers) for q in range(4)]
        packed = jnp.concatenate([recv[spot].astype(jnp.float32) for spot in spots], axis=0)
        blocks_in.append(block_transpose(packed, group, pair).astype(jnp.bfloat16))
    out_ref[...] = dot(jnp.concatenate(blocks_in, axis=1), weights[...])
    wait(send.at[pl.ds(0, peers - 1)], send_sem)
    up_bundle.wait_send()
    down_bundle.wait_send()


def body(projections, flats, block_start, bp_weights):
    rows, width = flats.shape
    peers = lax.axis_size("ang")
    weights = bp_weights.reshape(-1, bp_weights.shape[2])
    consts = [jnp.asarray(x) for x in tables(rows, width)]
    operands = [projections, flats, block_start, *consts, weights]
    blocks = width // LANES
    hbm = pl.BlockSpec(memory_space=pl.ANY)
    return pl.pallas_call(
        functools.partial(kernel, peers),
        out_shape=pltpu.VMEM((rows, weights.shape[1]), jnp.float32),
        in_specs=[hbm] * len(operands),
        out_specs=pl.BlockSpec(memory_space=pltpu.VMEM),
        scratch_shapes=[
            pltpu.VMEM(projections.shape, projections.dtype),
            pltpu.VMEM(flats.shape, flats.dtype),
            pltpu.SMEM(block_start.shape, block_start.dtype),
            *[pltpu.VMEM(x.shape, x.dtype) for x in (*consts, weights)],
            pltpu.VMEM((consts[0].shape[0], LANES), jnp.float32),
            pltpu.VMEM((2, blocks * HALO, LANES), jnp.bfloat16),
            pltpu.VMEM((2, blocks * HALO, LANES), jnp.bfloat16),
            pltpu.VMEM((blocks, rows, LANES), jnp.float32),
            pltpu.VMEM((peers, 2, LANES), jnp.bfloat16),
            pltpu.VMEM((peers, 2, LANES), jnp.bfloat16),
            pltpu.VMEM((peers // 4, 2, LANES), jnp.bfloat16),
            pltpu.VMEM((peers // 4 - 1, 2, LANES), jnp.bfloat16),
            pltpu.SemaphoreType.DMA((len(operands),)),
            pltpu.SemaphoreType.DMA((2,)),
            pltpu.SemaphoreType.DMA((2,)),
            pltpu.SemaphoreType.DMA,
            pltpu.SemaphoreType.DMA,
            pltpu.SemaphoreType.DMA((2,)),
            pltpu.SemaphoreType.DMA((2,)),
            pltpu.SemaphoreType.DMA((2,)),
            pltpu.SemaphoreType.REGULAR((2,)),
        ],
        compiler_params=pltpu.CompilerParams(collective_id=0, has_side_effects=True),
    )(*operands)


def solution(mesh):
    placed = (P(("scan", "ang"), "row", None), P(("scan", "row"), None), P(), P(None, None, "ang"))
    return jax.shard_map(
        body, mesh=mesh, in_specs=placed, out_specs=P(("scan", "row"), "ang"), check_vma=False
    )
```

```python
import functools

import jax
import jax.numpy as jnp
import numpy as np
from jax import lax
from jax.experimental import pallas as pl
from jax.experimental.pallas import tpu as pltpu
from jax.sharding import PartitionSpec as P

HALO = 4
LANES = 128
MESH = pl.DeviceIdType.MESH
paganin_beta = 8.0
ramp_gain = 320.0
NEAR = 2


def split(table):
    high = np.asarray(table, np.float32).astype(jnp.bfloat16)
    low = (np.asarray(table, np.float64) - high.astype(np.float64)).astype(np.float32).astype(jnp.bfloat16)
    return high, low


def tables(rows, width):
    blocks = width // LANES
    tile = rows + 2 * HALO
    half = blocks // 2
    t = np.arange(tile)
    basis, freqs = [np.full(tile, 1.0 / np.sqrt(tile))], [0]
    for u in range(1, tile // 2):
        basis += [np.sqrt(2.0 / tile) * np.cos(2 * np.pi * u * t / tile)]
        basis += [np.sqrt(2.0 / tile) * np.sin(2 * np.pi * u * t / tile)]
        freqs += [u, u]
    basis += [np.cos(np.pi * t) / np.sqrt(tile)]
    freqs += [tile // 2]
    basis, freqs = np.stack(basis), np.array(freqs)
    a, k = np.arange(blocks), np.arange(half + 1)
    turn = 2 * np.pi * np.outer(k, a) / blocks
    outer = np.concatenate([np.cos(turn), -np.sin(turn[1:half])])
    count = outer.shape[0] * tile

    def forward(cols):
        return np.einsum("ra,ut->ruat", outer, basis[:, cols]).reshape(count, -1)

    own = forward(slice(HALO, HALO + rows))
    halo = np.concatenate([forward(slice(0, HALO)), forward(slice(HALO + rows, tile))], axis=1)
    back = own.T
    b = np.arange(LANES)
    twist = 2 * np.pi * np.outer(k, b) / width
    wide = [np.repeat(x, 8, axis=0).astype(np.float32) for x in (np.cos(twist), np.sin(twist))]
    turn = 2 * np.pi * (np.outer(b, b) % LANES) / LANES
    c, s = np.cos(turn), np.sin(turn)
    inner = np.block([[c, -s], [s, c]])
    v = k[:, None] + blocks * b[None, :]
    lam = (4 * np.sin(np.pi * freqs / tile) ** 2)[None, :, None] + (4 * np.sin(np.pi * v / width) ** 2)[:, None, :]
    m = np.minimum(v, width - v)
    ramp = ramp_gain * (m / width) * (0.5 + 0.5 * np.cos(2 * np.pi * m / width))
    weight = np.where((k == 0) | (k == half), 1.0, 2.0)[:, None] / width
    gain = ((weight * ramp)[:, None, :] / (1 + paganin_beta * lam)).reshape(-1, LANES).astype(np.float32)
    own_h, own_l = split(own)
    halo_h, halo_l = split(halo)
    back_h, back_l = split(back)
    fore_h, fore_l = split(inner)
    hind_h, hind_l = split(inner.T)
    cat = functools.partial(np.concatenate, axis=1)
    return (
        cat([own_h, own_h, own_l]),
        cat([halo_h, halo_l]),
        np.stack(wide),
        np.stack([fore_h, fore_l]),
        gain,
        np.stack([hind_h, hind_l]),
        cat([back_h, back_h, back_l]),
    )


def halves(x):
    high = x.astype(jnp.bfloat16)
    return high, (x - high.astype(jnp.float32)).astype(jnp.bfloat16)


def dot(x, y):
    return jnp.dot(x, y, preferred_element_type=jnp.float32)


def data_times(x, table):
    high, low = halves(x)
    return dot(high, table[0]) + dot(low, table[0]) + dot(high, table[1])


def table_times(table, x):
    high, low = halves(x)
    return dot(table, jnp.concatenate([high, low, high], axis=0))


def block_transpose(x, group, pair):
    out = x
    for d in range(1, 4):
        moved = pltpu.roll(pltpu.roll(x, 32 * d, 1), 8 - 2 * d, 0)
        out = jnp.where((group - pair) % 4 == d, moved, out)
    return out


def kernel(
    peers,
    proj_hbm,
    flat_hbm,
    start_hbm,
    own_hbm,
    halo_hbm,
    wide_hbm,
    fore_hbm,
    gain_hbm,
    hind_hbm,
    back_hbm,
    weights_hbm,
    out_ref,
    proj,
    flat,
    starts,
    own_t,
    halo_t,
    wide,
    fore,
    gain,
    hind,
    back,
    weights,
    spread,
    edge,
    halo,
    sino,
    send,
    recv,
    relay_up,
    relay_down,
    load_sem,
    edge_sem,
    halo_sem,
    send_sem,
    recv_sem,
    relay_sem,
    bundle_send_sem,
    bundle_sem,
    round_sem,
):
    me = lax.axis_index("ang")
    row = lax.axis_index("row")
    row_count = lax.axis_size("row")
    rows, width = flat.shape
    blocks = width // LANES
    half = blocks // 2
    tile = rows + 2 * HALO

    def peer(d):
        return {"ang": lax.rem(me + (d + peers), peers)}

    def signal(sem, device):
        pl.semaphore_signal(sem, inc=1, device_id=device, device_id_type=MESH)

    loads = [
        pltpu.make_async_copy(src, dst, load_sem.at[i])
        for i, (src, dst) in enumerate(
            [
                (proj_hbm, proj),
                (flat_hbm, flat),
                (own_hbm, own_t),
                (halo_hbm, halo_t),
                (wide_hbm, wide),
                (fore_hbm, fore),
                (gain_hbm, gain),
                (hind_hbm, hind),
                (back_hbm, back),
                (start_hbm, starts),
                (weights_hbm, weights),
            ]
        )
    ]
    for load in loads[:2]:
        load.start()

    barrier = pltpu.get_barrier_semaphore()
    for d in range(1, NEAR + 1):
        signal(barrier, peer(d))
        signal(barrier, peer(-d))

    @pl.when(row > 0)
    def _():
        signal(barrier, {"row": row - 1})

    @pl.when(row < row_count - 1)
    def _():
        signal(barrier, {"row": row + 1})

    for load in loads[2:]:
        load.start()

    near = 2 * NEAR

    @pl.when((row > 0) & (row < row_count - 1))
    def _():
        pl.semaphore_wait(barrier, near + 2)

    @pl.when((row == 0) | (row == row_count - 1))
    def _():
        pl.semaphore_wait(barrier, near + 1)

    signal(round_sem.at[0], peer(NEAR))
    signal(round_sem.at[0], peer(-NEAR))

    sub = lax.broadcasted_iota(jnp.int32, (8, LANES), 0)
    lane = lax.broadcasted_iota(jnp.int32, (8, LANES), 1)
    loads[0].wait()
    loads[1].wait()
    contrast = []
    for a in range(blocks):
        cols = slice(a * LANES, (a + 1) * LANES)
        contrast.append(1.0 - proj[0, :, cols].astype(jnp.float32) / flat[:, cols])
    for a in range(0, blocks, 4):
        first, last = [], []
        for i in (a, a + 2):
            x, y = contrast[i], contrast[i + 1]
            first.append(jnp.where(sub < HALO, x, pltpu.roll(y, HALO, 0)))
            last.append(jnp.where(sub < HALO, pltpu.roll(x, HALO, 0), y))
        edge[0, a * HALO : (a + 4) * HALO, :] = jnp.concatenate(first, axis=0).astype(jnp.bfloat16)
        edge[1, a * HALO : (a + 4) * HALO, :] = jnp.concatenate(last, axis=0).astype(jnp.bfloat16)

    def edge_copy(which, to):
        return pltpu.make_async_remote_copy(
            src_ref=edge.at[which],
            dst_ref=halo.at[1 - which],
            send_sem=edge_sem.at[which],
            recv_sem=halo_sem.at[1 - which],
            device_id={"row": to},
            device_id_type=MESH,
        )

    up, down = edge_copy(0, row - 1), edge_copy(1, row + 1)

    @pl.when(row > 0)
    def _():
        up.start()

    @pl.when(row < row_count - 1)
    def _():
        down.start()

    @pl.when(row == 0)
    def _():
        halo[0] = jnp.zeros(halo.shape[1:], halo.dtype)

    @pl.when(row == row_count - 1)
    def _():
        halo[1] = jnp.zeros(halo.shape[1:], halo.dtype)

    loads[2].wait()
    spread[...] = table_times(own_t[...], jnp.concatenate(contrast, axis=0))

    pl.semaphore_wait(round_sem.at[0], 2)
    signal(round_sem.at[1], peer(2 * NEAR))
    signal(round_sem.at[1], peer(-2 * NEAR))

    for load in loads[3:-1]:
        load.wait()

    @pl.when(row > 0)
    def _():
        up.wait_send()
        pltpu.make_async_copy(halo.at[0], halo.at[0], halo_sem.at[0]).wait()

    @pl.when(row < row_count - 1)
    def _():
        down.wait_send()
        pltpu.make_async_copy(halo.at[1], halo.at[1], halo_sem.at[1]).wait()

    sides = jnp.concatenate([halo[0], halo[1]], axis=0)
    first = spread[...] + dot(halo_t[...], jnp.concatenate([sides, sides], axis=0))

    turn_re, turn_im = [], []
    for k in range(half + 1):
        c, s = wide[0, 8 * k : 8 * k + 8], wide[1, 8 * k : 8 * k + 8]
        for j in range(0, tile, 8):
            re = first[tile * k + j : tile * k + j + 8]
            if 0 < k < half:
                spot = tile * (half + k) + j
                im = first[spot : spot + 8]
                turn_re.append(re * c + im * s)
                turn_im.append(im * c - re * s)
            else:
                turn_re.append(re * c)
                turn_im.append(-(re * s))
    turned = jnp.concatenate([jnp.concatenate(turn_re, axis=0), jnp.concatenate(turn_im, axis=0)], axis=1)
    spectrum = data_times(turned, fore)
    scale = gain[...]
    spectrum = spectrum * jnp.concatenate([scale, scale], axis=1)
    undone = data_times(spectrum, hind)
    real, imag = [], []
    for k in range(half + 1):
        c, s = wide[0, 8 * k : 8 * k + 8], wide[1, 8 * k : 8 * k + 8]
        for j in range(0, tile, 8):
            re = undone[tile * k + j : tile * k + j + 8, :LANES]
            im = undone[tile * k + j : tile * k + j + 8, LANES:]
            real.append(re * c - im * s)
            if 0 < k < half:
                imag.append(im * c + re * s)
    filtered = table_times(back[...], jnp.concatenate(real + imag, axis=0))
    for a in range(blocks):
        sino[a] = filtered[8 * a : 8 * a + 8]

    group, pair = lane // 32, sub // 2
    for j in range(0, peers, 4):
        merged = None
        for q in range(4):
            begin = starts[me, j + q]
            a, b = begin // LANES, begin % LANES
            piece = jnp.where(lane >= b, sino[a], sino[jnp.minimum(a + 1, blocks - 1)])
            piece = pltpu.roll(piece, lax.rem(32 * q - b + LANES, LANES), 1)
            merged = piece if q == 0 else jnp.where(group == q, piece, merged)
        packed = block_transpose(merged, group, pair)
        for q in range(4):
            send[j + q] = packed[2 * q : 2 * q + 2].astype(jnp.bfloat16)

    far = peers // 4

    def hand(block, to, slot, sem):
        pltpu.make_async_remote_copy(
            src_ref=send.at[lax.rem(me + block + peers, peers)],
            dst_ref=slot,
            send_sem=send_sem,
            recv_sem=sem,
            device_id=peer(to),
            device_id_type=MESH,
        ).start()

    for d in range(1, far + 1):
        if d == 2 * NEAR + 1:
            pl.semaphore_wait(round_sem.at[1], 2)
        hand(d, d, recv.at[peers - d], recv_sem)
        hand(-d, -d, recv.at[d], recv_sem)
        hand(d + far, d, relay_up.at[far - d], relay_sem.at[0])
        if d < far:
            hand(-d - far, -d, relay_down.at[d - 1], relay_sem.at[1])
    recv[0] = send[me]

    def wait(ref, sem):
        pltpu.make_async_copy(ref, ref, sem).wait()

    def bundle(which, to, source, spots):
        return pltpu.make_async_remote_copy(
            src_ref=source,
            dst_ref=recv.at[spots],
            send_sem=bundle_send_sem.at[which],
            recv_sem=bundle_sem.at[which],
            device_id=peer(to),
            device_id_type=MESH,
        )

    up_bundle = bundle(0, far, relay_up, pl.ds(peers - 2 * far, far))
    down_bundle = bundle(1, -far, relay_down, pl.ds(far + 1, far - 1))

    def pass_up():
        wait(relay_up, relay_sem.at[0])
        up_bundle.start()

    def pass_down():
        wait(relay_down, relay_sem.at[1])
        down_bundle.start()

    @pl.when(me < peers // 2)
    def _():
        pass_down()
        pass_up()

    @pl.when(me >= peers // 2)
    def _():
        pass_up()
        pass_down()

    wait(recv.at[pl.ds(0, 2 * far)], recv_sem)
    up_bundle.wait_recv()
    down_bundle.wait_recv()
    loads[-1].wait()
    blocks_in = []
    for j in range(0, peers, 4):
        spots = [lax.rem(j + q + peers - me, peers) for q in range(4)]
        packed = jnp.concatenate([recv[spot].astype(jnp.float32) for spot in spots], axis=0)
        blocks_in.append(block_transpose(packed, group, pair).astype(jnp.bfloat16))
    out_ref[...] = dot(jnp.concatenate(blocks_in, axis=1), weights[...])
    wait(send.at[pl.ds(0, peers - 1)], send_sem)
    up_bundle.wait_send()
    down_bundle.wait_send()


def body(projections, flats, block_start, bp_weights):
    rows, width = flats.shape
    peers = lax.axis_size("ang")
    weights = bp_weights.reshape(-1, bp_weights.shape[2])
    consts = [jnp.asarray(x) for x in tables(rows, width)]
    operands = [projections, flats, block_start, *consts, weights]
    blocks = width // LANES
    hbm = pl.BlockSpec(memory_space=pl.ANY)
    return pl.pallas_call(
        functools.partial(kernel, peers),
        out_shape=pltpu.VMEM((rows, weights.shape[1]), jnp.float32),
        in_specs=[hbm] * len(operands),
        out_specs=pl.BlockSpec(memory_space=pltpu.VMEM),
        scratch_shapes=[
            pltpu.VMEM(projections.shape, projections.dtype),
            pltpu.VMEM(flats.shape, flats.dtype),
            pltpu.SMEM(block_start.shape, block_start.dtype),
            *[pltpu.VMEM(x.shape, x.dtype) for x in (*consts, weights)],
            pltpu.VMEM((consts[0].shape[0], LANES), jnp.float32),
            pltpu.VMEM((2, blocks * HALO, LANES), jnp.bfloat16),
            pltpu.VMEM((2, blocks * HALO, LANES), jnp.bfloat16),
            pltpu.VMEM((blocks, rows, LANES), jnp.float32),
            pltpu.VMEM((peers, 2, LANES), jnp.bfloat16),
            pltpu.VMEM((peers, 2, LANES), jnp.bfloat16),
            pltpu.VMEM((peers // 4, 2, LANES), jnp.bfloat16),
            pltpu.VMEM((peers // 4 - 1, 2, LANES), jnp.bfloat16),
            pltpu.SemaphoreType.DMA((len(operands),)),
            pltpu.SemaphoreType.DMA((2,)),
            pltpu.SemaphoreType.DMA((2,)),
            pltpu.SemaphoreType.DMA,
            pltpu.SemaphoreType.DMA,
            pltpu.SemaphoreType.DMA((2,)),
            pltpu.SemaphoreType.DMA((2,)),
            pltpu.SemaphoreType.DMA((2,)),
            pltpu.SemaphoreType.REGULAR((2,)),
        ],
        compiler_params=pltpu.CompilerParams(collective_id=0, has_side_effects=True),
    )(*operands)


def solution(mesh):
    placed = (P(("scan", "ang"), "row", None), P(("scan", "row"), None), P(), P(None, None, "ang"))
    return jax.shard_map(
        body, mesh=mesh, in_specs=placed, out_specs=P(("scan", "row"), "ang"), check_vma=False
    )
```

```python
import functools

import jax
import jax.numpy as jnp
import numpy as np
from jax import lax
from jax.experimental import pallas as pl
from jax.experimental.pallas import tpu as pltpu
from jax.sharding import PartitionSpec as P

HALO = 4
LANES = 128
MESH = pl.DeviceIdType.MESH
paganin_beta = 8.0
ramp_gain = 320.0
NEAR = 2


def split(table):
    high = np.asarray(table, np.float32).astype(jnp.bfloat16)
    low = (np.asarray(table, np.float64) - high.astype(np.float64)).astype(np.float32).astype(jnp.bfloat16)
    return high, low


def tables(rows, width):
    blocks = width // LANES
    tile = rows + 2 * HALO
    half = blocks // 2
    t = np.arange(tile)
    basis, freqs = [np.full(tile, 1.0 / np.sqrt(tile))], [0]
    for u in range(1, tile // 2):
        basis += [np.sqrt(2.0 / tile) * np.cos(2 * np.pi * u * t / tile)]
        basis += [np.sqrt(2.0 / tile) * np.sin(2 * np.pi * u * t / tile)]
        freqs += [u, u]
    basis += [np.cos(np.pi * t) / np.sqrt(tile)]
    freqs += [tile // 2]
    basis, freqs = np.stack(basis), np.array(freqs)
    a, k = np.arange(blocks), np.arange(half + 1)
    turn = 2 * np.pi * np.outer(k, a) / blocks
    outer = np.concatenate([np.cos(turn), -np.sin(turn[1:half])])
    count = outer.shape[0] * tile

    def forward(cols):
        return np.einsum("ra,ut->ruat", outer, basis[:, cols]).reshape(count, -1)

    own = forward(slice(HALO, HALO + rows))
    halo = np.concatenate([forward(slice(0, HALO)), forward(slice(HALO + rows, tile))], axis=1)
    back = own.T
    b = np.arange(LANES)
    twist = 2 * np.pi * np.outer(k, b) / width
    wide = [np.repeat(x, 8, axis=0).astype(np.float32) for x in (np.cos(twist), np.sin(twist))]
    turn = 2 * np.pi * (np.outer(b, b) % LANES) / LANES
    c, s = np.cos(turn), np.sin(turn)
    inner = np.block([[c, -s], [s, c]])
    v = k[:, None] + blocks * b[None, :]
    lam = (4 * np.sin(np.pi * freqs / tile) ** 2)[None, :, None] + (4 * np.sin(np.pi * v / width) ** 2)[:, None, :]
    m = np.minimum(v, width - v)
    ramp = ramp_gain * (m / width) * (0.5 + 0.5 * np.cos(2 * np.pi * m / width))
    weight = np.where((k == 0) | (k == half), 1.0, 2.0)[:, None] / width
    gain = ((weight * ramp)[:, None, :] / (1 + paganin_beta * lam)).reshape(-1, LANES).astype(np.float32)
    own_h, own_l = split(own)
    halo_h, halo_l = split(halo)
    back_h, back_l = split(back)
    fore_h, fore_l = split(inner)
    hind_h, hind_l = split(inner.T)
    cat = functools.partial(np.concatenate, axis=1)
    return (
        cat([own_h, own_h, own_l]),
        cat([halo_h, halo_l]),
        np.stack(wide),
        np.stack([fore_h, fore_l]),
        gain,
        np.stack([hind_h, hind_l]),
        cat([back_h, back_h, back_l]),
    )


def halves(x):
    high = x.astype(jnp.bfloat16)
    return high, (x - high.astype(jnp.float32)).astype(jnp.bfloat16)


def dot(x, y):
    return jnp.dot(x, y, preferred_element_type=jnp.float32)


def data_times(x, table):
    high, low = halves(x)
    return dot(high, table[0]) + dot(low, table[0]) + dot(high, table[1])


def table_times(table, x):
    high, low = halves(x)
    return dot(table, jnp.concatenate([high, low, high], axis=0))


def block_transpose(x, group, pair):
    out = x
    for d in range(1, 4):
        moved = pltpu.roll(pltpu.roll(x, 32 * d, 1), 8 - 2 * d, 0)
        out = jnp.where((group - pair) % 4 == d, moved, out)
    return out


def kernel(
    peers,
    proj_hbm,
    flat_hbm,
    start_hbm,
    own_hbm,
    halo_hbm,
    wide_hbm,
    fore_hbm,
    gain_hbm,
    hind_hbm,
    back_hbm,
    weights_hbm,
    out_ref,
    proj,
    flat,
    starts,
    own_t,
    halo_t,
    wide,
    fore,
    gain,
    hind,
    back,
    weights,
    spread,
    edge,
    halo,
    sino,
    send,
    recv,
    relay_up,
    relay_down,
    load_sem,
    edge_sem,
    halo_sem,
    send_sem,
    recv_sem,
    relay_sem,
    bundle_send_sem,
    bundle_sem,
    round_sem,
    row_sem,
):
    me = lax.axis_index("ang")
    row = lax.axis_index("row")
    row_count = lax.axis_size("row")
    rows, width = flat.shape
    blocks = width // LANES
    half = blocks // 2
    tile = rows + 2 * HALO

    def peer(d):
        return {"ang": lax.rem(me + (d + peers), peers)}

    def signal(sem, device):
        pl.semaphore_signal(sem, inc=1, device_id=device, device_id_type=MESH)

    loads = [
        pltpu.make_async_copy(src, dst, load_sem.at[i])
        for i, (src, dst) in enumerate(
            [
                (proj_hbm, proj),
                (flat_hbm, flat),
                (own_hbm, own_t),
                (halo_hbm, halo_t),
                (wide_hbm, wide),
                (fore_hbm, fore),
                (gain_hbm, gain),
                (hind_hbm, hind),
                (back_hbm, back),
                (start_hbm, starts),
                (weights_hbm, weights),
            ]
        )
    ]
    for load in loads[:2]:
        load.start()

    barrier = pltpu.get_barrier_semaphore()
    for d in range(1, NEAR + 1):

        @pl.when(me < peers - d)
        def _():
            signal(barrier, peer(d))

        @pl.when(me < d)
        def _():
            signal(barrier, peer(-d))

    @pl.when(row < row_count - 1)
    def _():
        signal(barrier, {"row": row + 1})

    for load in loads[2:]:
        load.start()

    greeted = jnp.minimum(me, NEAR) + jnp.maximum(me + NEAR + 1 - peers, 0)
    entered = greeted + jnp.minimum(row, 1)

    @pl.when(entered > 0)
    def _():
        pl.semaphore_wait(barrier, entered)

    @pl.when(row > 0)
    def _():
        signal(row_sem, {"row": row - 1})

    for d in range(1, NEAR + 1):

        @pl.when(me >= d)
        def _():
            signal(round_sem.at[2], peer(-d))

        @pl.when(me >= peers - d)
        def _():
            signal(round_sem.at[2], peer(d))

    sub = lax.broadcasted_iota(jnp.int32, (8, LANES), 0)
    lane = lax.broadcasted_iota(jnp.int32, (8, LANES), 1)
    loads[0].wait()
    loads[1].wait()
    contrast = []
    for a in range(blocks):
        cols = slice(a * LANES, (a + 1) * LANES)
        contrast.append(1.0 - proj[0, :, cols].astype(jnp.float32) / flat[:, cols])
    for a in range(0, blocks, 4):
        first, last = [], []
        for i in (a, a + 2):
            x, y = contrast[i], contrast[i + 1]
            first.append(jnp.where(sub < HALO, x, pltpu.roll(y, HALO, 0)))
            last.append(jnp.where(sub < HALO, pltpu.roll(x, HALO, 0), y))
        edge[0, a * HALO : (a + 4) * HALO, :] = jnp.concatenate(first, axis=0).astype(jnp.bfloat16)
        edge[1, a * HALO : (a + 4) * HALO, :] = jnp.concatenate(last, axis=0).astype(jnp.bfloat16)

    def edge_copy(which, to):
        return pltpu.make_async_remote_copy(
            src_ref=edge.at[which],
            dst_ref=halo.at[1 - which],
            send_sem=edge_sem.at[which],
            recv_sem=halo_sem.at[1 - which],
            device_id={"row": to},
            device_id_type=MESH,
        )

    up, down = edge_copy(0, row - 1), edge_copy(1, row + 1)

    @pl.when(row > 0)
    def _():
        up.start()

    @pl.when(row < row_count - 1)
    def _():
        pl.semaphore_wait(row_sem, 1)
        down.start()

    @pl.when(row == 0)
    def _():
        halo[0] = jnp.zeros(halo.shape[1:], halo.dtype)

    @pl.when(row == row_count - 1)
    def _():
        halo[1] = jnp.zeros(halo.shape[1:], halo.dtype)

    loads[2].wait()
    spread[...] = table_times(own_t[...], jnp.concatenate(contrast, axis=0))

    answers = 2 * NEAR - greeted

    @pl.when(answers > 0)
    def _():
        pl.semaphore_wait(round_sem.at[2], answers)

    signal(round_sem.at[0], peer(NEAR))
    signal(round_sem.at[0], peer(-NEAR))
    pl.semaphore_wait(round_sem.at[0], 2)
    signal(round_sem.at[1], peer(2 * NEAR))
    signal(round_sem.at[1], peer(-2 * NEAR))

    for load in loads[3:-1]:
        load.wait()

    @pl.when(row > 0)
    def _():
        up.wait_send()
        pltpu.make_async_copy(halo.at[0], halo.at[0], halo_sem.at[0]).wait()

    @pl.when(row < row_count - 1)
    def _():
        down.wait_send()
        pltpu.make_async_copy(halo.at[1], halo.at[1], halo_sem.at[1]).wait()

    sides = jnp.concatenate([halo[0], halo[1]], axis=0)
    first = spread[...] + dot(halo_t[...], jnp.concatenate([sides, sides], axis=0))

    turn_re, turn_im = [], []
    for k in range(half + 1):
        c, s = wide[0, 8 * k : 8 * k + 8], wide[1, 8 * k : 8 * k + 8]
        for j in range(0, tile, 8):
            re = first[tile * k + j : tile * k + j + 8]
            if 0 < k < half:
                spot = tile * (half + k) + j
                im = first[spot : spot + 8]
                turn_re.append(re * c + im * s)
                turn_im.append(im * c - re * s)
            else:
                turn_re.append(re * c)
                turn_im.append(-(re * s))
    turned = jnp.concatenate([jnp.concatenate(turn_re, axis=0), jnp.concatenate(turn_im, axis=0)], axis=1)
    spectrum = data_times(turned, fore)
    scale = gain[...]
    spectrum = spectrum * jnp.concatenate([scale, scale], axis=1)
    undone = data_times(spectrum, hind)
    real, imag = [], []
    for k in range(half + 1):
        c, s = wide[0, 8 * k : 8 * k + 8], wide[1, 8 * k : 8 * k + 8]
        for j in range(0, tile, 8):
            re = undone[tile * k + j : tile * k + j + 8, :LANES]
            im = undone[tile * k + j : tile * k + j + 8, LANES:]
            real.append(re * c - im * s)
            if 0 < k < half:
                imag.append(im * c + re * s)
    filtered = table_times(back[...], jnp.concatenate(real + imag, axis=0))
    for a in range(blocks):
        sino[a] = filtered[8 * a : 8 * a + 8]

    far = peers // 4
    group, pair = lane // 32, sub // 2

    def pack(offsets):
        merged = None
        for q, d in enumerate(offsets):
            begin = starts[me, lax.rem(me + d + peers, peers)]
            a, b = begin // LANES, begin % LANES
            piece = jnp.where(lane >= b, sino[a], sino[jnp.minimum(a + 1, blocks - 1)])
            piece = pltpu.roll(piece, lax.rem(32 * q - b + LANES, LANES), 1)
            merged = piece if q == 0 else jnp.where(group == q, piece, merged)
        packed = block_transpose(merged, group, pair)
        for q, d in enumerate(offsets):
            send[d % peers] = packed[2 * q : 2 * q + 2].astype(jnp.bfloat16)

    def hand(block, to, slot, sem):
        pltpu.make_async_remote_copy(
            src_ref=send.at[block % peers],
            dst_ref=slot,
            send_sem=send_sem,
            recv_sem=sem,
            device_id=peer(to),
            device_id_type=MESH,
        ).start()

    def near_up(d):
        hand(d, d, recv.at[peers - d], recv_sem)

    def near_down(d):
        hand(-d, -d, recv.at[d], recv_sem)

    def far_up(d):
        hand(d + far, d, relay_up.at[far - d], relay_sem.at[0])

    def far_down(d):
        if d < far:
            hand(-d - far, -d, relay_down.at[d - 1], relay_sem.at[1])

    def both_up(d):
        near_up(d)
        far_up(d)

    def wait(ref, sem):
        pltpu.make_async_copy(ref, ref, sem).wait()

    def bundle(which, to, source, spots):
        return pltpu.make_async_remote_copy(
            src_ref=source,
            dst_ref=recv.at[spots],
            send_sem=bundle_send_sem.at[which],
            recv_sem=bundle_sem.at[which],
            device_id=peer(to),
            device_id_type=MESH,
        )

    up_bundle = bundle(0, far, relay_up, pl.ds(peers - 2 * far, far))
    down_bundle = bundle(1, -far, relay_down, pl.ds(far + 1, far - 1))

    def pass_up():
        wait(relay_up, relay_sem.at[0])
        up_bundle.start()

    def pass_down():
        wait(relay_down, relay_sem.at[1])
        down_bundle.start()

    pack((1, 2, -1, -2))
    for d in range(1, NEAR + 1):
        near_up(d)
        near_down(d)
    pack((3, 4, -3, -4))
    for d in range(NEAR + 1, 2 * NEAR + 1):
        near_up(d)
        near_down(d)
    for d in range(far + 1, peers // 2, 4):
        pack((d, d + 1, d + 2, d + 3))
        pack(tuple(-e % peers if e < peers // 2 else 0 for e in (d, d + 1, d + 2, d + 3)))
        if d == far + 1:
            for e in range(1, 2 * NEAR + 1):
                far_up(e)
                far_down(e)
    for d in range(2 * NEAR + 1, far, 4):
        pack((d, d + 1, d + 2, d + 3))
        pack((-d, -d - 1, -d - 2, -d - 3))
    early = range(2 * NEAR + 1, 3 * NEAR + 1)
    for d in early:

        @pl.when((me + d >= peers) & (me + d < peers + NEAR))
        def _():
            both_up(d)

    pl.semaphore_wait(round_sem.at[1], 2)

    for d in range(2 * NEAR + 1, far + 1):
        near_down(d)
        far_down(d)
        if d in early:

            @pl.when((me + d < peers) | (me + d >= peers + NEAR))
            def _():
                both_up(d)

        else:
            both_up(d)
    recv[0] = send[0]

    @pl.when(me < peers // 2)
    def _():
        pass_down()
        pass_up()

    @pl.when(me >= peers // 2)
    def _():
        pass_up()
        pass_down()

    wait(recv.at[pl.ds(0, 2 * far)], recv_sem)
    up_bundle.wait_recv()
    down_bundle.wait_recv()
    loads[-1].wait()
    blocks_in = []
    for j in range(0, peers, 4):
        spots = [lax.rem(j + q + peers - me, peers) for q in range(4)]
        packed = jnp.concatenate([recv[spot].astype(jnp.float32) for spot in spots], axis=0)
        blocks_in.append(block_transpose(packed, group, pair).astype(jnp.bfloat16))
    out_ref[...] = dot(jnp.concatenate(blocks_in, axis=1), weights[...])
    wait(send.at[pl.ds(0, peers - 1)], send_sem)
    up_bundle.wait_send()
    down_bundle.wait_send()


def body(projections, flats, block_start, bp_weights):
    rows, width = flats.shape
    peers = lax.axis_size("ang")
    weights = bp_weights.reshape(-1, bp_weights.shape[2])
    consts = [jnp.asarray(x) for x in tables(rows, width)]
    operands = [projections, flats, block_start, *consts, weights]
    blocks = width // LANES
    hbm = pl.BlockSpec(memory_space=pl.ANY)
    return pl.pallas_call(
        functools.partial(kernel, peers),
        out_shape=pltpu.VMEM((rows, weights.shape[1]), jnp.float32),
        in_specs=[hbm] * len(operands),
        out_specs=pl.BlockSpec(memory_space=pltpu.VMEM),
        scratch_shapes=[
            pltpu.VMEM(projections.shape, projections.dtype),
            pltpu.VMEM(flats.shape, flats.dtype),
            pltpu.SMEM(block_start.shape, block_start.dtype),
            *[pltpu.VMEM(x.shape, x.dtype) for x in (*consts, weights)],
            pltpu.VMEM((consts[0].shape[0], LANES), jnp.float32),
            pltpu.VMEM((2, blocks * HALO, LANES), jnp.bfloat16),
            pltpu.VMEM((2, blocks * HALO, LANES), jnp.bfloat16),
            pltpu.VMEM((blocks, rows, LANES), jnp.float32),
            pltpu.VMEM((peers, 2, LANES), jnp.bfloat16),
            pltpu.VMEM((peers, 2, LANES), jnp.bfloat16),
            pltpu.VMEM((peers // 4, 2, LANES), jnp.bfloat16),
            pltpu.VMEM((peers // 4 - 1, 2, LANES), jnp.bfloat16),
            pltpu.SemaphoreType.DMA((len(operands),)),
            pltpu.SemaphoreType.DMA((2,)),
            pltpu.SemaphoreType.DMA((2,)),
            pltpu.SemaphoreType.DMA,
            pltpu.SemaphoreType.DMA,
            pltpu.SemaphoreType.DMA((2,)),
            pltpu.SemaphoreType.DMA((2,)),
            pltpu.SemaphoreType.DMA((2,)),
            pltpu.SemaphoreType.REGULAR((3,)),
            pltpu.SemaphoreType.REGULAR,
        ],
        compiler_params=pltpu.CompilerParams(collective_id=0, has_side_effects=True),
    )(*operands)


def solution(mesh):
    placed = (P(("scan", "ang"), "row", None), P(("scan", "row"), None), P(), P(None, None, "ang"))
    return jax.shard_map(
        body, mesh=mesh, in_specs=placed, out_specs=P(("scan", "row"), "ang"), check_vma=False
    )
```

```python
import functools

import jax
import jax.numpy as jnp
import numpy as np
from jax import lax
from jax.experimental import pallas as pl
from jax.experimental.pallas import tpu as pltpu
from jax.sharding import PartitionSpec as P

HALO = 4
LANES = 128
MESH = pl.DeviceIdType.MESH
paganin_beta = 8.0
ramp_gain = 320.0
NEAR = 2
ENDS = 3


def split(table):
    high = np.asarray(table, np.float32).astype(jnp.bfloat16)
    low = (np.asarray(table, np.float64) - high.astype(np.float64)).astype(np.float32).astype(jnp.bfloat16)
    return high, low


def tables(rows, width):
    blocks = width // LANES
    tile = rows + 2 * HALO
    half = blocks // 2
    t = np.arange(tile)
    basis, freqs = [np.full(tile, 1.0 / np.sqrt(tile))], [0]
    for u in range(1, tile // 2):
        basis += [np.sqrt(2.0 / tile) * np.cos(2 * np.pi * u * t / tile)]
        basis += [np.sqrt(2.0 / tile) * np.sin(2 * np.pi * u * t / tile)]
        freqs += [u, u]
    basis += [np.cos(np.pi * t) / np.sqrt(tile)]
    freqs += [tile // 2]
    basis, freqs = np.stack(basis), np.array(freqs)
    a, k = np.arange(blocks), np.arange(half + 1)
    turn = 2 * np.pi * np.outer(k, a) / blocks
    outer = np.concatenate([np.cos(turn), -np.sin(turn[1:half])])
    count = outer.shape[0] * tile

    def forward(cols):
        return np.einsum("ra,ut->ruat", outer, basis[:, cols]).reshape(count, -1)

    own = forward(slice(HALO, HALO + rows))
    halo = np.concatenate([forward(slice(0, HALO)), forward(slice(HALO + rows, tile))], axis=1)
    back = own.T
    b = np.arange(LANES)
    twist = 2 * np.pi * np.outer(k, b) / width
    wide = [np.repeat(x, 8, axis=0).astype(np.float32) for x in (np.cos(twist), np.sin(twist))]
    turn = 2 * np.pi * (np.outer(b, b) % LANES) / LANES
    c, s = np.cos(turn), np.sin(turn)
    inner = np.block([[c, -s], [s, c]])
    v = k[:, None] + blocks * b[None, :]
    lam = (4 * np.sin(np.pi * freqs / tile) ** 2)[None, :, None] + (4 * np.sin(np.pi * v / width) ** 2)[:, None, :]
    m = np.minimum(v, width - v)
    ramp = ramp_gain * (m / width) * (0.5 + 0.5 * np.cos(2 * np.pi * m / width))
    weight = np.where((k == 0) | (k == half), 1.0, 2.0)[:, None] / width
    gain = ((weight * ramp)[:, None, :] / (1 + paganin_beta * lam)).reshape(-1, LANES).astype(np.float32)
    own_h, own_l = split(own)
    halo_h, halo_l = split(halo)
    back_h, back_l = split(back)
    fore_h, fore_l = split(inner)
    hind_h, hind_l = split(inner.T)
    cat = functools.partial(np.concatenate, axis=1)
    return (
        cat([own_h, own_h, own_l]),
        cat([halo_h, halo_l]),
        np.stack(wide),
        np.stack([fore_h, fore_l]),
        gain,
        np.stack([hind_h, hind_l]),
        cat([back_h, back_h, back_l]),
    )


def halves(x):
    high = x.astype(jnp.bfloat16)
    return high, (x - high.astype(jnp.float32)).astype(jnp.bfloat16)


def dot(x, y):
    return jnp.dot(x, y, preferred_element_type=jnp.float32)


def data_times(x, table):
    high, low = halves(x)
    return dot(high, table[0]) + dot(low, table[0]) + dot(high, table[1])


def table_times(table, x):
    high, low = halves(x)
    return dot(table, jnp.concatenate([high, low, high], axis=0))


def block_transpose(x, group, pair):
    out = x
    for d in range(1, 4):
        moved = pltpu.roll(pltpu.roll(x, 32 * d, 1), 8 - 2 * d, 0)
        out = jnp.where((group - pair) % 4 == d, moved, out)
    return out


def kernel(
    peers,
    proj_hbm,
    flat_hbm,
    start_hbm,
    own_hbm,
    halo_hbm,
    wide_hbm,
    fore_hbm,
    gain_hbm,
    hind_hbm,
    back_hbm,
    weights_hbm,
    out_ref,
    proj,
    flat,
    starts,
    own_t,
    halo_t,
    wide,
    fore,
    gain,
    hind,
    back,
    weights,
    spread,
    edge,
    halo,
    sino,
    send,
    recv,
    relay_up,
    relay_down,
    load_sem,
    edge_sem,
    halo_sem,
    send_sem,
    recv_sem,
    relay_sem,
    bundle_send_sem,
    bundle_sem,
    round_sem,
    row_sem,
):
    me = lax.axis_index("ang")
    row = lax.axis_index("row")
    row_count = lax.axis_size("row")
    rows, width = flat.shape
    blocks = width // LANES
    half = blocks // 2
    tile = rows + 2 * HALO

    def peer(d):
        return {"ang": lax.rem(me + (d + peers), peers)}

    def signal(sem, device):
        pl.semaphore_signal(sem, inc=1, device_id=device, device_id_type=MESH)

    loads = [
        pltpu.make_async_copy(src, dst, load_sem.at[i])
        for i, (src, dst) in enumerate(
            [
                (proj_hbm, proj),
                (flat_hbm, flat),
                (own_hbm, own_t),
                (halo_hbm, halo_t),
                (wide_hbm, wide),
                (fore_hbm, fore),
                (gain_hbm, gain),
                (hind_hbm, hind),
                (back_hbm, back),
                (start_hbm, starts),
                (weights_hbm, weights),
            ]
        )
    ]
    for load in loads[:2]:
        load.start()

    barrier = pltpu.get_barrier_semaphore()
    for d in range(1, NEAR + 1):

        @pl.when(me < peers - d)
        def _():
            signal(barrier, peer(d))

    for d in range(1, ENDS + 1):

        @pl.when(me < d)
        def _():
            signal(barrier, peer(-d))

    @pl.when(row < row_count - 1)
    def _():
        signal(barrier, {"row": row + 1})

    greeted = jnp.minimum(me, NEAR) + jnp.maximum(me + ENDS + 1 - peers, 0)
    entered = greeted + jnp.minimum(row, 1)

    @pl.when(entered > 0)
    def _():
        pl.semaphore_wait(barrier, entered)

    @pl.when(row > 0)
    def _():
        signal(row_sem, {"row": row - 1})

    for d in range(1, NEAR + 1):

        @pl.when(me >= d)
        def _():
            signal(round_sem.at[2], peer(-d))

    for d in range(1, ENDS + 1):

        @pl.when(me >= peers - d)
        def _():
            signal(round_sem.at[2], peer(d))

    answers = jnp.minimum(peers - 1 - me, NEAR) + jnp.maximum(ENDS - me, 0)

    def first_round():
        @pl.when(answers > 0)
        def _():
            pl.semaphore_wait(round_sem.at[2], answers)

        signal(round_sem.at[0], peer(NEAR))
        signal(round_sem.at[0], peer(-NEAR))

    @pl.when(me >= peers - NEAR)
    def _():
        first_round()

    sub = lax.broadcasted_iota(jnp.int32, (8, LANES), 0)
    lane = lax.broadcasted_iota(jnp.int32, (8, LANES), 1)
    loads[0].wait()
    loads[1].wait()
    for load in loads[2:]:
        load.start()
    contrast = []
    for a in range(blocks):
        cols = slice(a * LANES, (a + 1) * LANES)
        contrast.append(1.0 - proj[0, :, cols].astype(jnp.float32) / flat[:, cols])
    for a in range(0, blocks, 4):
        first, last = [], []
        for i in (a, a + 2):
            x, y = contrast[i], contrast[i + 1]
            first.append(jnp.where(sub < HALO, x, pltpu.roll(y, HALO, 0)))
            last.append(jnp.where(sub < HALO, pltpu.roll(x, HALO, 0), y))
        edge[0, a * HALO : (a + 4) * HALO, :] = jnp.concatenate(first, axis=0).astype(jnp.bfloat16)
        edge[1, a * HALO : (a + 4) * HALO, :] = jnp.concatenate(last, axis=0).astype(jnp.bfloat16)

    def edge_copy(which, to):
        return pltpu.make_async_remote_copy(
            src_ref=edge.at[which],
            dst_ref=halo.at[1 - which],
            send_sem=edge_sem.at[which],
            recv_sem=halo_sem.at[1 - which],
            device_id={"row": to},
            device_id_type=MESH,
        )

    up, down = edge_copy(0, row - 1), edge_copy(1, row + 1)

    @pl.when(row > 0)
    def _():
        up.start()

    @pl.when(row < row_count - 1)
    def _():
        pl.semaphore_wait(row_sem, 1)
        down.start()

    @pl.when(row == 0)
    def _():
        halo[0] = jnp.zeros(halo.shape[1:], halo.dtype)

    @pl.when(row == row_count - 1)
    def _():
        halo[1] = jnp.zeros(halo.shape[1:], halo.dtype)

    loads[2].wait()
    spread[...] = table_times(own_t[...], jnp.concatenate(contrast, axis=0))

    @pl.when(me < peers - NEAR)
    def _():
        first_round()

    pl.semaphore_wait(round_sem.at[0], 2)
    signal(round_sem.at[1], peer(2 * NEAR))
    signal(round_sem.at[1], peer(-2 * NEAR))

    for load in loads[3:-1]:
        load.wait()

    @pl.when(row > 0)
    def _():
        up.wait_send()
        pltpu.make_async_copy(halo.at[0], halo.at[0], halo_sem.at[0]).wait()

    @pl.when(row < row_count - 1)
    def _():
        down.wait_send()
        pltpu.make_async_copy(halo.at[1], halo.at[1], halo_sem.at[1]).wait()

    sides = jnp.concatenate([halo[0], halo[1]], axis=0)
    first = spread[...] + dot(halo_t[...], jnp.concatenate([sides, sides], axis=0))

    turn_re, turn_im = [], []
    for k in range(half + 1):
        c, s = wide[0, 8 * k : 8 * k + 8], wide[1, 8 * k : 8 * k + 8]
        for j in range(0, tile, 8):
            re = first[tile * k + j : tile * k + j + 8]
            if 0 < k < half:
                spot = tile * (half + k) + j
                im = first[spot : spot + 8]
                turn_re.append(re * c + im * s)
                turn_im.append(im * c - re * s)
            else:
                turn_re.append(re * c)
                turn_im.append(-(re * s))
    turned = jnp.concatenate([jnp.concatenate(turn_re, axis=0), jnp.concatenate(turn_im, axis=0)], axis=1)
    spectrum = data_times(turned, fore)
    scale = gain[...]
    spectrum = spectrum * jnp.concatenate([scale, scale], axis=1)
    undone = data_times(spectrum, hind)
    real, imag = [], []
    for k in range(half + 1):
        c, s = wide[0, 8 * k : 8 * k + 8], wide[1, 8 * k : 8 * k + 8]
        for j in range(0, tile, 8):
            re = undone[tile * k + j : tile * k + j + 8, :LANES]
            im = undone[tile * k + j : tile * k + j + 8, LANES:]
            real.append(re * c - im * s)
            if 0 < k < half:
                imag.append(im * c + re * s)
    filtered = table_times(back[...], jnp.concatenate(real + imag, axis=0))
    for a in range(blocks):
        sino[a] = filtered[8 * a : 8 * a + 8]

    far = peers // 4
    group, pair = lane // 32, sub // 2

    def pack(offsets):
        merged = None
        for q, d in enumerate(offsets):
            begin = starts[me, lax.rem(me + d + peers, peers)]
            a, b = begin // LANES, begin % LANES
            piece = jnp.where(lane >= b, sino[a], sino[jnp.minimum(a + 1, blocks - 1)])
            piece = pltpu.roll(piece, lax.rem(32 * q - b + LANES, LANES), 1)
            merged = piece if q == 0 else jnp.where(group == q, piece, merged)
        packed = block_transpose(merged, group, pair)
        for q, d in enumerate(offsets):
            send[d % peers] = packed[2 * q : 2 * q + 2].astype(jnp.bfloat16)

    def hand(block, to, slot, sem):
        pltpu.make_async_remote_copy(
            src_ref=send.at[block % peers],
            dst_ref=slot,
            send_sem=send_sem,
            recv_sem=sem,
            device_id=peer(to),
            device_id_type=MESH,
        ).start()

    def near_up(d):
        hand(d, d, recv.at[peers - d], recv_sem)

    def near_down(d):
        hand(-d, -d, recv.at[d], recv_sem)

    def far_up(d):
        hand(d + far, d, relay_up.at[far - d], relay_sem.at[0])

    def far_down(d):
        if d < far:
            hand(-d - far, -d, relay_down.at[d - 1], relay_sem.at[1])

    def both_up(d):
        near_up(d)
        far_up(d)

    def wait(ref, sem):
        pltpu.make_async_copy(ref, ref, sem).wait()

    def bundle(which, to, source, spots):
        return pltpu.make_async_remote_copy(
            src_ref=source,
            dst_ref=recv.at[spots],
            send_sem=bundle_send_sem.at[which],
            recv_sem=bundle_sem.at[which],
            device_id=peer(to),
            device_id_type=MESH,
        )

    up_bundle = bundle(0, far, relay_up, pl.ds(peers - 2 * far, far))
    down_bundle = bundle(1, -far, relay_down, pl.ds(far + 1, far - 1))

    def pass_up():
        wait(relay_up, relay_sem.at[0])
        up_bundle.start()

    def pass_down():
        wait(relay_down, relay_sem.at[1])
        down_bundle.start()

    pack((1, 2, 3, 4))
    for d in range(1, 2 * NEAR + 1):
        near_up(d)
    pack((9, 10, 11, 12))
    for d in range(1, 2 * NEAR + 1):
        far_up(d)
    pack((-1, -2, -3, -4))
    for d in range(1, 2 * NEAR + 1):
        near_down(d)
    pack((-9, -10, -11, -12))
    for d in range(1, 2 * NEAR + 1):
        far_down(d)
    pack((13, 14, 15, 16))
    pack((-13, -14, -15, 0))
    for d in range(2 * NEAR + 1, far, 4):
        pack((d, d + 1, d + 2, d + 3))
        pack((-d, -d - 1, -d - 2, -d - 3))
    early = range(2 * NEAR + 1, 2 * NEAR + ENDS + 1)
    for d in early:

        @pl.when((me + d >= peers) & (me + d < peers + ENDS))
        def _():
            both_up(d)

    pl.semaphore_wait(round_sem.at[1], 2)

    for d in range(2 * NEAR + 1, far + 1):
        near_down(d)
        far_down(d)
        if d in early:

            @pl.when((me + d < peers) | (me + d >= peers + ENDS))
            def _():
                both_up(d)

        else:
            both_up(d)
    recv[0] = send[0]

    @pl.when(me < peers // 2)
    def _():
        pass_down()
        pass_up()

    @pl.when(me >= peers // 2)
    def _():
        pass_up()
        pass_down()

    wait(recv.at[pl.ds(0, 2 * far)], recv_sem)
    up_bundle.wait_recv()
    down_bundle.wait_recv()
    loads[-1].wait()
    blocks_in = []
    for j in range(0, peers, 4):
        spots = [lax.rem(j + q + peers - me, peers) for q in range(4)]
        packed = jnp.concatenate([recv[spot].astype(jnp.float32) for spot in spots], axis=0)
        blocks_in.append(block_transpose(packed, group, pair).astype(jnp.bfloat16))
    out_ref[...] = dot(jnp.concatenate(blocks_in, axis=1), weights[...])
    wait(send.at[pl.ds(0, peers - 1)], send_sem)
    up_bundle.wait_send()
    down_bundle.wait_send()


def body(projections, flats, block_start, bp_weights):
    rows, width = flats.shape
    peers = lax.axis_size("ang")
    weights = bp_weights.reshape(-1, bp_weights.shape[2])
    consts = [jnp.asarray(x) for x in tables(rows, width)]
    operands = [projections, flats, block_start, *consts, weights]
    blocks = width // LANES
    hbm = pl.BlockSpec(memory_space=pl.ANY)
    return pl.pallas_call(
        functools.partial(kernel, peers),
        out_shape=pltpu.VMEM((rows, weights.shape[1]), jnp.float32),
        in_specs=[hbm] * len(operands),
        out_specs=pl.BlockSpec(memory_space=pltpu.VMEM),
        scratch_shapes=[
            pltpu.VMEM(projections.shape, projections.dtype),
            pltpu.VMEM(flats.shape, flats.dtype),
            pltpu.SMEM(block_start.shape, block_start.dtype),
            *[pltpu.VMEM(x.shape, x.dtype) for x in (*consts, weights)],
            pltpu.VMEM((consts[0].shape[0], LANES), jnp.float32),
            pltpu.VMEM((2, blocks * HALO, LANES), jnp.bfloat16),
            pltpu.VMEM((2, blocks * HALO, LANES), jnp.bfloat16),
            pltpu.VMEM((blocks, rows, LANES), jnp.float32),
            pltpu.VMEM((peers, 2, LANES), jnp.bfloat16),
            pltpu.VMEM((peers, 2, LANES), jnp.bfloat16),
            pltpu.VMEM((peers // 4, 2, LANES), jnp.bfloat16),
            pltpu.VMEM((peers // 4 - 1, 2, LANES), jnp.bfloat16),
            pltpu.SemaphoreType.DMA((len(operands),)),
            pltpu.SemaphoreType.DMA((2,)),
            pltpu.SemaphoreType.DMA((2,)),
            pltpu.SemaphoreType.DMA,
            pltpu.SemaphoreType.DMA,
            pltpu.SemaphoreType.DMA((2,)),
            pltpu.SemaphoreType.DMA((2,)),
            pltpu.SemaphoreType.DMA((2,)),
            pltpu.SemaphoreType.REGULAR((3,)),
            pltpu.SemaphoreType.REGULAR,
        ],
        compiler_params=pltpu.CompilerParams(collective_id=0, has_side_effects=True),
    )(*operands)


def solution(mesh):
    placed = (P(("scan", "ang"), "row", None), P(("scan", "row"), None), P(), P(None, None, "ang"))
    return jax.shard_map(
        body, mesh=mesh, in_specs=placed, out_specs=P(("scan", "row"), "ang"), check_vma=False
    )
```
